256 devices in a mesh: shift: 4 (over y_lo, core), band: 4 (over z_lo), lane: 16 (over z_hi, y_hi, x).
Axes of the slice: x: 4, y: 4 (y_hi: 2, y_lo: 2; y = y_hi * 2 + y_lo), z: 8 (z_hi: 2, z_lo: 4; z = z_hi * 4 + z_lo), core: 2. Of those that a mesh axis runs over, the one named last changes fastest.
Arguments:
- source_terms: float32 [1024, 1024, 128], P(('shift', 'band'), 'lane'), parts along dimension 0, may hold values from -6 to 6
- initial_values: float32 [1024, 1024, 128], P(('shift', 'band'), 'lane'), parts along dimension 0, may hold values from -6 to 6
- absorption: float32 [1024, 1024, 128], P(('shift', 'band'), 'lane'), parts along dimension 0, may hold values from 0.1 to 0.9
Outputs:
- corrected: float32 [1024, 1024, 128], P(('shift', 'band'), 'lane'), parts along dimension 0
The draws below stay inside these ranges and needn't reach their ends.
There are 4 independent parts, one for each index of `shift`. The reference program is written for one: setup_inputs(seed, part) draws one part's arguments, and reference() takes and returns one part's arrays. A program takes and returns all parts, laid end to end along the dimension named above; each array names one. Nothing has to cross between parts.
All inputs are finite; a program needn't handle non-finite values.
Results may differ from the reference program's by a relative error of at most 0.0003.
Values sent between devices are 32-bit elements.
A program may use at most 64 MiB of HBM per device.

```python
import jax
import jax.numpy as jnp
from jax import lax

CASES = 128
RATIO = 2
BEFORE = 3
AFTER = 3
INNER = 13
GRID_Y = 256
GRID_X = 1024


def level_of(key, extent, pieces, low, largest):
    loudness, own = 1.0, jax.random.fold_in(key, 6)
    for axis_at, shards_of in pieces:
        heights = jnp.exp(jax.random.uniform(jax.random.fold_in(own, axis_at), (shards_of,), jnp.float32, low / len(pieces), largest / len(pieces)))
        loudness = loudness * jnp.repeat(heights, extent[axis_at] // shards_of).reshape([-1 if axis == axis_at else 1 for axis in range(len(extent))])
    return loudness


def noise(stream_key, extent, spread, bound, split=(), held_as=jnp.bfloat16):
    drawn = spread * jax.random.normal(stream_key, extent, jnp.float32)
    if split:
        drawn = drawn * level_of(stream_key, extent, split, -0.22, 0.18)
    return jnp.clip(drawn, -bound, bound).astype(held_as)


def setup_inputs(seed: int = 0, part: int = 0) -> dict:
    arg_keys = jax.random.split(jax.random.key(seed), 4)
    part_keys = jax.random.split(jax.random.fold_in(arg_keys[3], part), 4)
    source_terms = noise(part_keys[0], (GRID_Y, GRID_X, CASES), 1.0, 6.0, ((0, 4), (1, 16)), jnp.float32)
    initial_values = noise(part_keys[1], (GRID_Y, GRID_X, CASES), 1.0, 6.0, ((0, 4), (1, 16)), jnp.float32)
    absorption = jnp.clip(0.1 + 0.79999997 * jax.random.uniform(part_keys[2], (GRID_Y, GRID_X, CASES), jnp.float32) ** level_of(part_keys[2], (GRID_Y, GRID_X, CASES), ((0, 4), (1, 16)), -0.2, 0.2), 0.1, 0.9)
    return {"source_terms": source_terms, "initial_values": initial_values, "absorption": absorption}


def neighbour_sum(padded):
    inner_y, inner_x = padded.shape[0] - 2, padded.shape[1] - 2
    middle_rows = lax.slice_in_dim(padded, 1, 1 + inner_y, axis=0)
    middle_columns = lax.slice_in_dim(padded, 1, 1 + inner_x, axis=1)
    return (lax.slice_in_dim(middle_columns, 0, inner_y, axis=0) + lax.slice_in_dim(middle_columns, 2, 2 + inner_y, axis=0)
            + lax.slice_in_dim(middle_rows, 0, inner_x, axis=1) + lax.slice_in_dim(middle_rows, 2, 2 + inner_x, axis=1))


def sweep_once(padded, values, load, mass_here):
    return values + 0.8 * (load + neighbour_sum(padded) - (4.0 + mass_here) * values) / (4.0 + mass_here)


def block_means(values):
    cut = values.reshape(values.shape[0] // RATIO, RATIO, values.shape[1] // RATIO, RATIO, values.shape[2])
    return jnp.mean(cut, axis=(1, 3))


def spread_blocks(values):
    return jnp.repeat(jnp.repeat(values, RATIO, axis=0), RATIO, axis=1)


def reference(source_terms, initial_values, absorption):
    values = initial_values
    for sweep in range(BEFORE):
        values = sweep_once(jnp.pad(values, ((1, 1), (1, 1), (0, 0)), mode="constant"), values, source_terms, absorption)
    defect = source_terms + neighbour_sum(jnp.pad(values, ((1, 1), (1, 1), (0, 0)), mode="constant")) - (4.0 + absorption) * values
    coarse_load, coarse_mass = block_means(defect) * RATIO, block_means(absorption) * RATIO
    coarse_values = jnp.zeros_like(coarse_load)
    for sweep in range(INNER):
        coarse_values = sweep_once(jnp.pad(coarse_values, ((1, 1), (1, 1), (0, 0)), mode="constant"), coarse_values, coarse_load, coarse_mass)
    values = values + spread_blocks(coarse_values)
    for sweep in range(AFTER):
        values = sweep_once(jnp.pad(values, ((1, 1), (1, 1), (0, 0)), mode="constant"), values, source_terms, absorption)
    corrected = values
    return corrected
```

```python
import jax
import jax.numpy as jnp
from jax import lax
from jax.experimental import pallas as pl
from jax.experimental.pallas import tpu as pltpu
from jax.sharding import PartitionSpec as P

CASES = 128
BEFORE = 3
AFTER = 3
INNER = 13
N = 64
M = N // 2
DU = BEFORE + 1
DW = BEFORE
DV = AFTER
DC = INNER + 1
DM = INNER

PF, YF, XF = 88, 4, 8
SIZE_F = (N + 2 * YF) * PF
PC, YC, XC = 72, 14, 16
SIZE_C = (M + 2 * YC) * PC

SIDES = ((0, -1), (0, 1), (-1, 0), (1, 0), (-1, -1), (-1, 1), (1, -1), (1, 1))
MESH = pl.DeviceIdType.MESH


class Grid:
    def __init__(self, size, pitch, y_off, x_off):
        self.size, self.pitch, self.y_off, self.x_off = size, pitch, y_off, x_off

    def at(self, y, x):
        return (y + self.y_off) * self.pitch + x + self.x_off


FINE = Grid(N, PF, YF, XF)
COARSE = Grid(M, PC, YC, XC)


def pieces(grid, side, depth, sending):
    sy, sx = side
    n = grid.size

    def span(sign, count):
        if sending:
            return n - count if sign > 0 else 0
        return n if sign > 0 else -count

    if sy == 0:
        x0 = span(sx, depth)
        return [(grid.at(0, x0 + i), n, grid.pitch) for i in range(depth)]
    if sx == 0:
        y0 = span(sy, depth)
        return [(grid.at(y0 + i, 0), n, 1) for i in range(depth)]
    runs = []
    for dx in range(1, depth):
        if sending:
            x = n - dx if sx > 0 else dx - 1
        else:
            x = n - 1 + dx if sx > 0 else -dx
        count = depth - dx
        runs.append((grid.at(span(sy, count), x), count, grid.pitch))
    return runs


def message_rows(parts, side):
    total = sum(
        count for grid, depth in parts for _, count, _ in pieces(grid, side, depth, True)
    )
    return -(-total // 8) * 8


def rows(start, count, stride):
    return pl.ds(start, count) if stride == 1 else pl.ds(start, count, stride=stride)


def pack(buffer, refs, parts, side):
    at = 0
    for ref, (grid, depth) in zip(refs, parts):
        for start, count, stride in pieces(grid, side, depth, True):
            buffer[pl.ds(at, count), :] = ref[rows(start, count, stride), :]
            at += count


def unpack(buffer, refs, parts, side):
    at = 0
    for ref, (grid, depth) in zip(refs, parts):
        for start, count, stride in pieces(grid, side, depth, False):
            ref[rows(start, count, stride), :] = buffer[pl.ds(at, count), :]
            at += count


def clear(ref, grid, side, depth):
    sy, sx = side
    n = grid.size
    if sy == 0:
        for i in range(depth):
            x = n + i if sx > 0 else -1 - i
            count = n + 2 * grid.y_off
            ref[pl.ds(grid.at(-grid.y_off, x), count, stride=grid.pitch), :] = jnp.zeros(
                (count, CASES), jnp.float32
            )
    else:
        y0 = n if sy > 0 else -depth
        count = depth * grid.pitch
        ref[pl.ds(grid.at(y0, -grid.x_off), count), :] = jnp.zeros((count, CASES), jnp.float32)


PART_A = ((FINE, DU), (FINE, DW), (FINE, DW))
PART_M = ((COARSE, DM),)
PART_B = ((COARSE, DC),)
PART_V = ((FINE, DV),)
STAGES = (PART_A, PART_M, PART_B, PART_V)


def sweep(grid, src, dst, gain, base, groups, y_low, y_high, store_at=None, unroll=4):
    store_at = store_at or grid.at
    blocks = -(-(y_high - y_low) // unroll)

    def block(i, carry):
        y = jnp.minimum(y_low + i * unroll, y_high - unroll)
        row = grid.at(y, 0)
        out_row = store_at(y, 0)
        out_pitch = store_at(1, 0) - store_at(0, 0)
        for x0, width in groups:

            def load(ref, dy, x):
                return ref[pl.ds(row + dy * grid.pitch + x0 + x, 8, stride=width), :]

            left = [load(src, k, -1) for k in range(unroll)]
            here = [load(src, k, 0) for k in range(unroll)]
            for x in range(width):
                right = [load(src, k, x + 1) for k in range(unroll)]
                above = load(src, -1, x)
                below = load(src, unroll, x)
                for k in range(unroll):
                    up = here[k - 1] if k else above
                    down = here[k + 1] if k + 1 < unroll else below
                    around = (left[k] + right[k]) + (up + down)
                    new = (
                        0.2 * here[k] + load(base, k, x) + load(gain, k, x) * around
                    )
                    dst[pl.ds(out_row + k * out_pitch + x0 + x, 8, stride=width), :] = new
                left, here = here, right
        return carry

    lax.fori_loop(0, blocks, block, 0)


def kernel(source_hbm, values_hbm, mass_hbm, out_ref, source, start, mass, u0, u1, gain, base,
           coarse_gain, c0, c1, coarse_base, *rest):
    counts = len(STAGES) * len(SIDES)
    send_bufs, recv_bufs = rest[:counts], rest[counts : 2 * counts]
    load_sem, send_sem, recv_sem = rest[2 * counts :]
    band, lane = lax.axis_index("band"), lax.axis_index("lane")
    bands, lanes = lax.axis_size("band"), lax.axis_size("lane")

    loads = [
        pltpu.make_async_copy(src, dst, load_sem.at[i])
        for i, (src, dst) in enumerate(
            ((mass_hbm, mass), (source_hbm, source), (values_hbm, start))
        )
    ]
    for copy in loads:
        copy.start()

    exists, targets = [], []
    for sy, sx in SIDES:
        y, x = band + sy, lane + sx
        exists.append((y >= 0) & (y < bands) & (x >= 0) & (x < lanes))
        targets.append({"band": y, "lane": x})

    barrier = pltpu.get_barrier_semaphore()
    for there, target in zip(exists, targets):

        @pl.when(there)
        def _():
            pl.semaphore_signal(barrier, inc=1, device_id=target, device_id_type=MESH)

    for k in range(4):

        @pl.when(jnp.logical_not(exists[k]))
        def _():
            for ref, grid, depth in (
                (u0, FINE, DU), (gain, FINE, DW), (base, FINE, DW),
                (coarse_gain, COARSE, DM), (coarse_base, COARSE, DC),
            ):
                clear(ref, grid, SIDES[k], depth)

    loads[0].wait()

    def coarse_row(y, carry):
        for x in range(0, M, 8):
            total = None
            for dy in range(2):
                for dx in range(2):
                    part = mass[pl.ds((2 * y + dy) * N + 2 * x + dx, 8, stride=2), :]
                    total = part if total is None else total + part
            at = pl.multiple_of(COARSE.at(y, x), 8)
            coarse_gain[pl.ds(at, 8), :] = 0.8 / (4.0 + 0.5 * total)
        return carry

    lax.fori_loop(0, M, coarse_row, 0)
    loads[1].wait()
    loads[2].wait()

    def fine_row(y, carry):
        for x in range(0, N, 8):
            here = pl.ds(pl.multiple_of(y * N + x, 8), 8)
            there = pl.ds(pl.multiple_of(FINE.at(y, x), 8), 8)
            factor = 0.8 / (4.0 + mass[here, :])
            gain[there, :] = factor
            base[there, :] = factor * source[here, :]
            u0[there, :] = start[here, :]
        return carry

    lax.fori_loop(0, N, fine_row, 0)

    def copy_of(stage, k, arriving=False):
        at = stage * len(SIDES) + k
        sy, sx = SIDES[k]
        over = at if arriving else stage * len(SIDES) + SIDES.index((-sy, -sx))
        return pltpu.make_async_remote_copy(
            send_bufs[at], recv_bufs[over], send_sem.at[at], recv_sem.at[over],
            device_id=targets[k], device_id_type=MESH,
        )

    def send(stage, refs):
        for k, side in enumerate(SIDES):

            @pl.when(exists[k])
            def _():
                pack(send_bufs[stage * len(SIDES) + k], refs, STAGES[stage], side)
                copy_of(stage, k).start()

    def receive(stage, refs):
        for k, side in enumerate(SIDES):

            @pl.when(exists[k])
            def _():
                copy_of(stage, k, arriving=True).wait_recv()
                unpack(recv_bufs[stage * len(SIDES) + k], refs, STAGES[stage], side)

    total = jnp.int32(0)
    for there in exists:
        total = total + there.astype(jnp.int32)
    pl.semaphore_wait(barrier, total)

    send(0, (u0, gain, base))
    send(1, (coarse_gain,))
    receive(0, (u0, gain, base))

    wide = ((-DU, 9),)
    sweep(FINE, u0, u1, gain, base, wide, -3, N + 3)
    sweep(FINE, u1, u0, gain, base, wide, -2, N + 2)
    sweep(FINE, u0, u1, gain, base, wide, -1, N + 1)

    def restrict_row(y, carry):
        for x in range(0, M, 8):

            def u_at(dy, dx):
                return u1[pl.ds(FINE.at(2 * y + dy, 2 * x + dx), 8, stride=2), :]

            def own(ref, dy, dx):
                return ref[pl.ds((2 * y + dy) * N + 2 * x + dx, 8, stride=2), :]

            block = {}
            for dy in range(2):
                for dx in range(2):
                    block[dy, dx] = u_at(dy, dx)
            total = None
            for dy in range(2):
                for dx in range(2):
                    here = block[dy, dx]
                    around = (u_at(dy, -1 if dx == 0 else 2) + u_at(-1 if dy == 0 else 2, dx)) + (
                        block[dy, 1 - dx] + block[1 - dy, dx]
                    )
                    defect = (own(source, dy, dx) + around) - (4.0 + own(mass, dy, dx)) * here
                    total = defect if total is None else total + defect
            at = pl.multiple_of(COARSE.at(y, x), 8)
            coarse_base[pl.ds(at, 8), :] = coarse_gain[pl.ds(at, 8), :] * (0.5 * total)
        return carry

    lax.fori_loop(0, M, restrict_row, 0)
    send(2, (coarse_base,))
    send(3, (u1,))
    receive(1, (coarse_gain,))
    receive(2, (coarse_base,))

    src, dst = coarse_base, c0
    for step in range(1, INNER):
        depth = DC - step
        span = M + 2 * depth
        if span > 56:
            groups = ((-depth, 4), (-depth + 32, 4))
        else:
            groups = ((-depth, -(-span // 8)),)
        sweep(COARSE, src, dst, coarse_gain, coarse_base, groups, -depth, M + depth)
        src, dst = dst, (c1 if dst is c0 else c0)
    coarse = src

    for k in range(4):

        @pl.when(jnp.logical_not(exists[k]))
        def _():
            clear(u1, FINE, SIDES[k], DV)

    receive(3, (u1,))

    def prolong_row(i, carry):
        y = i - 2
        for x in (-2, 6, 14, 22, M - 6):
            add = coarse[pl.ds(COARSE.at(y, x), 8), :]
            for dy in range(2):
                for dx in range(2):
                    at = pl.ds(FINE.at(2 * y + dy, 2 * x + dx), 8, stride=2)
                    u0[at, :] = u1[at, :] + add
        return carry

    lax.fori_loop(0, M + 4, prolong_row, 0)
    sweep(FINE, u0, u1, gain, base, wide, -2, N + 2)
    sweep(FINE, u1, u0, gain, base, wide, -1, N + 1)
    sweep(FINE, u0, out_ref, gain, base, ((0, 4), (32, 4)), 0, N, store_at=lambda y, x: y * N + x)

    for stage in range(len(STAGES)):
        for k in range(len(SIDES)):

            @pl.when(exists[k])
            def _():
                copy_of(stage, k).wait_send()


def per_device(source_terms, initial_values, absorption):
    shape = source_terms.shape
    flat = [x.reshape(N * N, CASES) for x in (source_terms, initial_values, absorption)]
    vmem = lambda count: pltpu.VMEM((count, CASES), jnp.float32)
    buffers = [vmem(message_rows(parts, side)) for parts in STAGES for side in SIDES]
    result = pl.pallas_call(
        kernel,
        out_shape=jax.ShapeDtypeStruct((N * N, CASES), jnp.float32),
        in_specs=[pl.BlockSpec(memory_space=pl.ANY)] * 3,
        out_specs=pl.BlockSpec(memory_space=pltpu.VMEM),
        scratch_shapes=[vmem(N * N)] * 3
        + [vmem(SIZE_F)] * 4
        + [vmem(SIZE_C)] * 4
        + buffers
        + buffers
        + [
            pltpu.SemaphoreType.DMA((3,)),
            pltpu.SemaphoreType.DMA((len(buffers),)),
            pltpu.SemaphoreType.DMA((len(buffers),)),
        ],
        compiler_params=pltpu.CompilerParams(
            collective_id=0, has_side_effects=True, vmem_limit_bytes=56 << 20
        ),
        name="cycle",
    )(*flat)
    return result.reshape(shape)


def solution(mesh):
    placed = P(("shift", "band"), "lane", None)
    return jax.shard_map(
        per_device,
        mesh=mesh,
        in_specs=(placed,) * 3,
        out_specs=placed,
        check_vma=False,
    )
```

```python
import jax
import jax.numpy as jnp
from jax import lax
from jax.experimental import pallas as pl
from jax.experimental.pallas import tpu as pltpu
from jax.sharding import PartitionSpec as P

CASES = 128
BEFORE = 3
AFTER = 3
INNER = 13
N = 64
M = N // 2
DU = BEFORE + 1
DW = BEFORE
DV = AFTER
DC = INNER + 1
DM = INNER

PF, YF, XF = 88, 4, 8
SIZE_F = (N + 2 * YF) * PF
PC, YC, XC = 72, 14, 16
SIZE_C = (M + 2 * YC) * PC

SLOW = ((7, 1, 3), (8, 0, 12))
CHUNKS = (3, 3, 3, 1)

SIDES = ((0, -1), (0, 1), (-1, 0), (1, 0), (-1, -1), (-1, 1), (1, -1), (1, 1))
MESH = pl.DeviceIdType.MESH


def split(stage):
    whole = message_rows(STAGES[stage], (0, 1))
    corners = 2 * message_rows(STAGES[stage], (1, 1))
    each = (whole + corners) // 2 // CHUNKS[stage] // 8 * 8
    first = whole - each * CHUNKS[stage]
    return first, [(first + i * each, each) for i in range(CHUNKS[stage])]


class Grid:
    def __init__(self, size, pitch, y_off, x_off):
        self.size, self.pitch, self.y_off, self.x_off = size, pitch, y_off, x_off

    def at(self, y, x):
        return (y + self.y_off) * self.pitch + x + self.x_off


FINE = Grid(N, PF, YF, XF)
COARSE = Grid(M, PC, YC, XC)


def pieces(grid, side, depth, sending):
    sy, sx = side
    n = grid.size

    def span(sign, count):
        if sending:
            return n - count if sign > 0 else 0
        return n if sign > 0 else -count

    if sy == 0:
        x0 = span(sx, depth)
        return [(grid.at(0, x0 + i), n, grid.pitch) for i in range(depth)]
    if sx == 0:
        y0 = span(sy, depth)
        return [(grid.at(y0 + i, 0), n, 1) for i in range(depth)]
    runs = []
    for dx in range(1, depth):
        if sending:
            x = n - dx if sx > 0 else dx - 1
        else:
            x = n - 1 + dx if sx > 0 else -dx
        count = depth - dx
        runs.append((grid.at(span(sy, count), x), count, grid.pitch))
    return runs


def message_rows(parts, side):
    total = sum(
        count for grid, depth in parts for _, count, _ in pieces(grid, side, depth, True)
    )
    return -(-total // 8) * 8


def rows(start, count, stride):
    return pl.ds(start, count) if stride == 1 else pl.ds(start, count, stride=stride)


def pack(buffer, refs, parts, side):
    at = 0
    for ref, (grid, depth) in zip(refs, parts):
        for start, count, stride in pieces(grid, side, depth, True):
            buffer[pl.ds(at, count), :] = ref[rows(start, count, stride), :]
            at += count


def unpack(buffer, refs, parts, side):
    at = 0
    for ref, (grid, depth) in zip(refs, parts):
        for start, count, stride in pieces(grid, side, depth, False):
            ref[rows(start, count, stride), :] = buffer[pl.ds(at, count), :]
            at += count


def clear(ref, grid, side, depth):
    sy, sx = side
    n = grid.size
    if sy == 0:
        for i in range(depth):
            x = n + i if sx > 0 else -1 - i
            count = n + 2 * grid.y_off
            ref[pl.ds(grid.at(-grid.y_off, x), count, stride=grid.pitch), :] = jnp.zeros(
                (count, CASES), jnp.float32
            )
    else:
        y0 = n if sy > 0 else -depth
        count = depth * grid.pitch
        ref[pl.ds(grid.at(y0, -grid.x_off), count), :] = jnp.zeros((count, CASES), jnp.float32)


PART_A = ((FINE, DU), (FINE, DW), (FINE, DW))
PART_M = ((COARSE, DM),)
PART_B = ((COARSE, DC),)
PART_V = ((FINE, DV),)
STAGES = (PART_A, PART_M, PART_B, PART_V)


def sweep(grid, src, dst, gain, base, groups, y_low, y_high, store_at=None, unroll=4):
    store_at = store_at or grid.at
    blocks = -(-(y_high - y_low) // unroll)

    def block(i, carry):
        y = jnp.minimum(y_low + i * unroll, y_high - unroll)
        row = grid.at(y, 0)
        out_row = store_at(y, 0)
        out_pitch = store_at(1, 0) - store_at(0, 0)
        for x0, width in groups:

            def load(ref, dy, x):
                return ref[pl.ds(row + dy * grid.pitch + x0 + x, 8, stride=width), :]

            left = [load(src, k, -1) for k in range(unroll)]
            here = [load(src, k, 0) for k in range(unroll)]
            for x in range(width):
                right = [load(src, k, x + 1) for k in range(unroll)]
                above = load(src, -1, x)
                below = load(src, unroll, x)
                for k in range(unroll):
                    up = here[k - 1] if k else above
                    down = here[k + 1] if k + 1 < unroll else below
                    around = (left[k] + right[k]) + (up + down)
                    new = (
                        0.2 * here[k] + load(base, k, x) + load(gain, k, x) * around
                    )
                    dst[pl.ds(out_row + k * out_pitch + x0 + x, 8, stride=width), :] = new
                left, here = here, right
        return carry

    lax.fori_loop(0, blocks, block, 0)


def kernel(source_hbm, values_hbm, mass_hbm, out_ref, source, start, mass, u0, u1, gain, base,
           coarse_gain, c0, c1, coarse_base, *rest):
    counts = len(STAGES) * len(SIDES)
    send_bufs, recv_bufs = rest[:counts], rest[counts : 2 * counts]
    held = rest[2 * counts : 2 * counts + len(STAGES)]
    load_sem, send_sem, recv_sem, hop_sems = rest[2 * counts + len(STAGES) :]
    band, lane = lax.axis_index("band"), lax.axis_index("lane")
    bands, lanes = lax.axis_size("band"), lax.axis_size("lane")

    loads = [
        pltpu.make_async_copy(src, dst, load_sem.at[i])
        for i, (src, dst) in enumerate(
            ((mass_hbm, mass), (source_hbm, source), (values_hbm, start))
        )
    ]
    for copy in loads:
        copy.start()

    exists, targets = [], []
    for sy, sx in SIDES:
        y, x = band + sy, lane + sx
        exists.append((y >= 0) & (y < bands) & (x >= 0) & (x < lanes))
        targets.append({"band": y, "lane": x})

    barrier = pltpu.get_barrier_semaphore()
    for there, target in zip(exists, targets):

        @pl.when(there)
        def _():
            pl.semaphore_signal(barrier, inc=1, device_id=target, device_id_type=MESH)

    for far, side, between in SLOW:
        other = far + (1 if side else -1)

        @pl.when(lane == between)
        def _():
            pl.semaphore_signal(barrier, inc=1, device_id={"lane": jnp.int32(far)}, device_id_type=MESH)

        @pl.when(lane == other)
        def _():
            pl.semaphore_signal(barrier, inc=1, device_id={"lane": jnp.int32(between)}, device_id_type=MESH)

    for k in range(4):

        @pl.when(jnp.logical_not(exists[k]))
        def _():
            for ref, grid, depth in (
                (u0, FINE, DU), (gain, FINE, DW), (base, FINE, DW),
                (coarse_gain, COARSE, DM), (coarse_base, COARSE, DC),
            ):
                clear(ref, grid, SIDES[k], depth)

    loads[0].wait()

    def coarse_row(y, carry):
        for x in range(0, M, 8):
            total = None
            for dy in range(2):
                for dx in range(2):
                    part = mass[pl.ds((2 * y + dy) * N + 2 * x + dx, 8, stride=2), :]
                    total = part if total is None else total + part
            at = pl.multiple_of(COARSE.at(y, x), 8)
            coarse_gain[pl.ds(at, 8), :] = 0.8 / (4.0 + 0.5 * total)
        return carry

    lax.fori_loop(0, M, coarse_row, 0)
    loads[1].wait()
    loads[2].wait()

    def fine_row(y, carry):
        for x in range(0, N, 8):
            here = pl.ds(pl.multiple_of(y * N + x, 8), 8)
            there = pl.ds(pl.multiple_of(FINE.at(y, x), 8), 8)
            factor = 0.8 / (4.0 + mass[here, :])
            gain[there, :] = factor
            base[there, :] = factor * source[here, :]
            u0[there, :] = start[here, :]
        return carry

    lax.fori_loop(0, N, fine_row, 0)

    def copy_of(stage, k, arriving=False):
        at = stage * len(SIDES) + k
        sy, sx = SIDES[k]
        over = at if arriving else stage * len(SIDES) + SIDES.index((-sy, -sx))
        return pltpu.make_async_remote_copy(
            send_bufs[at], recv_bufs[over], send_sem.at[at], recv_sem.at[over],
            device_id=targets[k], device_id_type=MESH,
        )

    hops = [(stage, i) for stage in range(len(STAGES)) for i in range(CHUNKS[stage])]

    def hop(stage, i, source_of, target, lane_to, leg):
        at = hops.index((stage, i))
        return pltpu.make_async_remote_copy(
            source_of, target, hop_sems.at[leg, 0, at], hop_sems.at[leg, 1, at],
            device_id={"lane": jnp.int32(lane_to)}, device_id_type=MESH,
        )

    def hops_of(leg, stage, far, side, between):
        first, chunks = split(stage)
        other = far + (1 if side else -1)
        out = []
        for i, (start, count) in enumerate(chunks):
            here = held[stage].at[pl.ds(start - first, count)]
            if leg == 0:
                sent = send_bufs[stage * len(SIDES) + side].at[pl.ds(start, count)]
                out.append(hop(stage, i, sent, here, between, 0))
            else:
                got = recv_bufs[stage * len(SIDES) + 1 - side].at[pl.ds(start, count)]
                out.append(hop(stage, i, here, got, other, 1))
        return out

    def straight(stage, k, arriving=False):
        at = stage * len(SIDES) + k
        over = at if arriving else at + 1 - 2 * k
        part = pl.ds(0, split(stage)[0])
        return pltpu.make_async_remote_copy(
            send_bufs[at].at[part], recv_bufs[over].at[part], send_sem.at[at], recv_sem.at[over],
            device_id=targets[k], device_id_type=MESH,
        )

    slow = [lane == far for far, _, _ in SLOW]
    slow_side = {side: i for i, (_, side, _) in enumerate(SLOW)}
    whole = [
        there & jnp.logical_not(slow[slow_side[k]]) if k in slow_side else there
        for k, there in enumerate(exists)
    ]

    def send(stage, refs):
        for k in (1, 0, 4, 5, 6, 7, 2, 3):

            @pl.when(exists[k])
            def _():
                pack(send_bufs[stage * len(SIDES) + k], refs, STAGES[stage], SIDES[k])

            if k in slow_side:

                @pl.when(slow[slow_side[k]])
                def _():
                    for first in hops_of(0, stage, *SLOW[slow_side[k]]):
                        first.start()
                    straight(stage, k).start()

            @pl.when(whole[k])
            def _():
                copy_of(stage, k).start()

    def pass_on(stage):
        for entry in SLOW:

            @pl.when(lane == entry[2])
            def _():
                for first, second in zip(hops_of(0, stage, *entry), hops_of(1, stage, *entry)):
                    first.wait_recv()
                    second.start()

    def receive(stage, refs):
        for k in (2, 3, 4, 5, 6, 7, 0, 1):
            if k in slow_side:

                @pl.when(slow[slow_side[k]])
                def _():
                    straight(stage, k, arriving=True).wait_recv()
                    for second in hops_of(1, stage, *SLOW[1 - slow_side[k]]):
                        second.wait_recv()

            @pl.when(whole[k])
            def _():
                copy_of(stage, k, arriving=True).wait_recv()

            @pl.when(exists[k])
            def _():
                unpack(recv_bufs[stage * len(SIDES) + k], refs, STAGES[stage], SIDES[k])

    total = jnp.int32(0)
    for there in exists:
        total = total + there.astype(jnp.int32)
    for far, _, between in SLOW:
        total = total + (lane == far).astype(jnp.int32) + (lane == between).astype(jnp.int32)
    pl.semaphore_wait(barrier, total)

    send(0, (u0, gain, base))
    send(1, (coarse_gain,))
    pass_on(0)
    pass_on(1)
    receive(0, (u0, gain, base))

    wide = ((-DU, 9),)
    sweep(FINE, u0, u1, gain, base, wide, -3, N + 3)
    sweep(FINE, u1, u0, gain, base, wide, -2, N + 2)
    sweep(FINE, u0, u1, gain, base, wide, -1, N + 1)

    def restrict_row(y, carry):
        for x in range(0, M, 8):

            def u_at(dy, dx):
                return u1[pl.ds(FINE.at(2 * y + dy, 2 * x + dx), 8, stride=2), :]

            def own(ref, dy, dx):
                return ref[pl.ds((2 * y + dy) * N + 2 * x + dx, 8, stride=2), :]

            block = {}
            for dy in range(2):
                for dx in range(2):
                    block[dy, dx] = u_at(dy, dx)
            total = None
            for dy in range(2):
                for dx in range(2):
                    here = block[dy, dx]
                    around = (u_at(dy, -1 if dx == 0 else 2) + u_at(-1 if dy == 0 else 2, dx)) + (
                        block[dy, 1 - dx] + block[1 - dy, dx]
                    )
                    defect = (own(source, dy, dx) + around) - (4.0 + own(mass, dy, dx)) * here
                    total = defect if total is None else total + defect
            at = pl.multiple_of(COARSE.at(y, x), 8)
            coarse_base[pl.ds(at, 8), :] = coarse_gain[pl.ds(at, 8), :] * (0.5 * total)
        return carry

    lax.fori_loop(0, M, restrict_row, 0)
    send(2, (coarse_base,))
    send(3, (u1,))
    pass_on(2)
    pass_on(3)
    receive(1, (coarse_gain,))
    receive(2, (coarse_base,))

    src, dst = coarse_base, c0
    for step in range(1, INNER):
        depth = DC - step
        span = M + 2 * depth
        if span > 56:
            groups = ((-depth, 4), (-depth + 32, 4))
        else:
            groups = ((-depth, -(-span // 8)),)
        sweep(COARSE, src, dst, coarse_gain, coarse_base, groups, -depth, M + depth)
        src, dst = dst, (c1 if dst is c0 else c0)
    coarse = src

    for k in range(4):

        @pl.when(jnp.logical_not(exists[k]))
        def _():
            clear(u1, FINE, SIDES[k], DV)

    receive(3, (u1,))

    def prolong_row(i, carry):
        y = i - 2
        for x in (-2, 6, 14, 22, M - 6):
            add = coarse[pl.ds(COARSE.at(y, x), 8), :]
            for dy in range(2):
                for dx in range(2):
                    at = pl.ds(FINE.at(2 * y + dy, 2 * x + dx), 8, stride=2)
                    u0[at, :] = u1[at, :] + add
        return carry

    lax.fori_loop(0, M + 4, prolong_row, 0)
    sweep(FINE, u0, u1, gain, base, wide, -2, N + 2)
    sweep(FINE, u1, u0, gain, base, wide, -1, N + 1)
    sweep(FINE, u0, out_ref, gain, base, ((0, 4), (32, 4)), 0, N, store_at=lambda y, x: y * N + x)

    for stage in range(len(STAGES)):
        for k in range(len(SIDES)):

            if k in slow_side:

                @pl.when(slow[slow_side[k]])
                def _():
                    for first in hops_of(0, stage, *SLOW[slow_side[k]]):
                        first.wait_send()
                    straight(stage, k).wait_send()

            @pl.when(whole[k])
            def _():
                copy_of(stage, k).wait_send()

        for entry in SLOW:

            @pl.when(lane == entry[2])
            def _():
                for second in hops_of(1, stage, *entry):
                    second.wait_send()


def per_device(source_terms, initial_values, absorption):
    shape = source_terms.shape
    flat = [x.reshape(N * N, CASES) for x in (source_terms, initial_values, absorption)]
    vmem = lambda count: pltpu.VMEM((count, CASES), jnp.float32)
    buffers = [vmem(message_rows(parts, side)) for parts in STAGES for side in SIDES]
    result = pl.pallas_call(
        kernel,
        out_shape=jax.ShapeDtypeStruct((N * N, CASES), jnp.float32),
        in_specs=[pl.BlockSpec(memory_space=pl.ANY)] * 3,
        out_specs=pl.BlockSpec(memory_space=pltpu.VMEM),
        scratch_shapes=[vmem(N * N)] * 3
        + [vmem(SIZE_F)] * 4
        + [vmem(SIZE_C)] * 4
        + buffers
        + buffers
        + [vmem(sum(count for _, count in split(stage)[1])) for stage in range(len(STAGES))]
        + [
            pltpu.SemaphoreType.DMA((3,)),
            pltpu.SemaphoreType.DMA((len(buffers),)),
            pltpu.SemaphoreType.DMA((len(buffers),)),
            pltpu.SemaphoreType.DMA((2, 2, sum(CHUNKS))),
        ],
        compiler_params=pltpu.CompilerParams(
            collective_id=0, has_side_effects=True, vmem_limit_bytes=56 << 20
        ),
        name="cycle",
    )(*flat)
    return result.reshape(shape)


def solution(mesh):
    placed = P(("shift", "band"), "lane", None)
    return jax.shard_map(
        per_device,
        mesh=mesh,
        in_specs=(placed,) * 3,
        out_specs=placed,
        check_vma=False,
    )
```

```python
import jax
import jax.numpy as jnp
from jax import lax
from jax.experimental import pallas as pl
from jax.experimental.pallas import tpu as pltpu
from jax.sharding import PartitionSpec as P

CASES = 128
BEFORE = 3
AFTER = 3
INNER = 13
N = 64
M = N // 2
DU = BEFORE + 1
DW = BEFORE
DV = AFTER
DC = INNER + 1
DM = INNER

PF, YF, XF = 88, 4, 8
SIZE_F = (N + 2 * YF) * PF
PC, YC, XC = 72, 14, 16
SIZE_C = (M + 2 * YC) * PC

SLOW = ((7, 1, 3), (8, 0, 12))
CHUNKS = (3, 2, 2, 0, 0)

SIDES = ((0, -1), (0, 1), (-1, 0), (1, 0), (-1, -1), (-1, 1), (1, -1), (1, 1))
MESH = pl.DeviceIdType.MESH


def split(stage):
    whole = message_rows(STAGES[stage], (0, 1))
    corners = 2 * message_rows(STAGES[stage], (1, 1))
    if not CHUNKS[stage]:
        return whole, []
    each = (whole + corners) // 2 // CHUNKS[stage] // 8 * 8
    first = whole - each * CHUNKS[stage]
    return first, [(first + i * each, each) for i in range(CHUNKS[stage])]


class Grid:
    def __init__(self, size, pitch, y_off, x_off):
        self.size, self.pitch, self.y_off, self.x_off = size, pitch, y_off, x_off

    def at(self, y, x):
        return (y + self.y_off) * self.pitch + x + self.x_off


FINE = Grid(N, PF, YF, XF)
COARSE = Grid(M, PC, YC, XC)


def runs(grid, side, boxes, sending):
    def place(sign, low, high):
        n = grid.size
        if sign == 0:
            return low, high - low
        if sending:
            return (n - high if sign > 0 else low - 1), high - low + 1
        return (n - 1 + low if sign > 0 else -high), high - low + 1

    out = []
    for y_range, x_range, along_x in boxes:
        y, height = place(side[0], *y_range)
        x, width = place(side[1], *x_range)
        if along_x:
            out += [(grid.at(y + i, x), width, 1) for i in range(height)]
        else:
            out += [(grid.at(y, x + i), height, grid.pitch) for i in range(width)]
    return out


def whole_halo(grid, side, depth):
    own = (0, grid.size)
    if side[0] == 0:
        return [(own, (1, depth), False)]
    if side[1] == 0:
        return [((1, depth), own, True)]
    return [((1, depth - dx), (dx, dx), False) for dx in range(1, depth)]


RIM = 2


def early_halo(grid, side, depth):
    own, deep = (RIM, grid.size - RIM), (RIM + 1, depth)
    if side[0] == 0:
        return [(own, deep, False)]
    if side[1] == 0:
        return [(deep, own, True)]
    return [((RIM + 1, depth - dx), (dx, dx), False) for dx in range(RIM + 1, depth - RIM)]


def late_halo(grid, side, depth):
    n = grid.size
    own, near, deep = (0, n), (1, RIM), (RIM + 1, depth)
    ends = [(0, RIM), (n - RIM, n)]
    if side[0] == 0:
        return [(own, near, False)] + [(end, deep, True) for end in ends]
    if side[1] == 0:
        return [(near, own, True)] + [(deep, end, False) for end in ends]
    return [((1, depth - dx), (dx, dx), False) for dx in range(1, RIM + 1)] + [
        ((dy, dy), (RIM + 1, depth - dy), True) for dy in range(1, RIM + 1)
    ]


def pieces(part, side, sending):
    grid, depth, boxes = part
    return runs(grid, side, boxes(grid, side, depth), sending)


def message_rows(parts, side):
    total = sum(
        count for part in parts for _, count, _ in pieces(part, side, True)
    )
    return -(-total // 8) * 8


def rows(start, count, stride):
    return pl.ds(start, count) if stride == 1 else pl.ds(start, count, stride=stride)


def pack(buffer, refs, parts, side):
    at = 0
    for ref, part in zip(refs, parts):
        for start, count, stride in pieces(part, side, True):
            buffer[pl.ds(at, count), :] = ref[rows(start, count, stride), :]
            at += count


def unpack(buffer, refs, parts, side):
    at = 0
    for ref, part in zip(refs, parts):
        for start, count, stride in pieces(part, side, False):
            ref[rows(start, count, stride), :] = buffer[pl.ds(at, count), :]
            at += count


def clear(ref, grid, side, depth):
    sy, sx = side
    n = grid.size
    if sy == 0:
        for i in range(depth):
            x = n + i if sx > 0 else -1 - i
            count = n + 2 * grid.y_off
            ref[pl.ds(grid.at(-grid.y_off, x), count, stride=grid.pitch), :] = jnp.zeros(
                (count, CASES), jnp.float32
            )
    else:
        y0 = n if sy > 0 else -depth
        count = depth * grid.pitch
        ref[pl.ds(grid.at(y0, -grid.x_off), count), :] = jnp.zeros((count, CASES), jnp.float32)


STAGES = (
    ((FINE, DU, whole_halo), (FINE, DW, whole_halo), (FINE, DW, whole_halo)),
    ((COARSE, DM, whole_halo),),
    ((COARSE, DC, early_halo),),
    ((COARSE, DC, late_halo),),
    ((FINE, DV, whole_halo),),
)


def sweep(grid, src, dst, gain, base, groups, y_low, y_high, store_at=None, unroll=4):
    store_at = store_at or grid.at
    blocks = -(-(y_high - y_low) // unroll)

    def block(i, carry):
        y = jnp.minimum(y_low + i * unroll, y_high - unroll)
        row = grid.at(y, 0)
        out_row = store_at(y, 0)
        out_pitch = store_at(1, 0) - store_at(0, 0)
        for x0, width in groups:

            def load(ref, dy, x):
                return ref[pl.ds(row + dy * grid.pitch + x0 + x, 8, stride=width), :]

            left = [load(src, k, -1) for k in range(unroll)]
            here = [load(src, k, 0) for k in range(unroll)]
            for x in range(width):
                right = [load(src, k, x + 1) for k in range(unroll)]
                above = load(src, -1, x)
                below = load(src, unroll, x)
                for k in range(unroll):
                    up = here[k - 1] if k else above
                    down = here[k + 1] if k + 1 < unroll else below
                    around = (left[k] + right[k]) + (up + down)
                    new = (
                        0.2 * here[k] + load(base, k, x) + load(gain, k, x) * around
                    )
                    dst[pl.ds(out_row + k * out_pitch + x0 + x, 8, stride=width), :] = new
                left, here = here, right
        return carry

    lax.fori_loop(0, blocks, block, 0)


def sweep_strip(grid, src, dst, gain, base, x0, width):
    def block(i, carry):
        row = grid.at(8 * i, x0)

        def load(ref, dy, x):
            return ref[pl.ds(row + dy * grid.pitch + x, 8, stride=grid.pitch), :]

        left, here = load(src, 0, -1), load(src, 0, 0)
        for x in range(width):
            right = load(src, 0, x + 1)
            around = (left + right) + (load(src, -1, x) + load(src, 1, x))
            new = 0.2 * here + load(base, 0, x) + load(gain, 0, x) * around
            dst[pl.ds(row + x, 8, stride=grid.pitch), :] = new
            left, here = here, right
        return carry

    lax.fori_loop(0, grid.size // 8, block, 0)


def kernel(source_hbm, values_hbm, mass_hbm, out_ref, source, start, mass, u0, u1, u2, u3, gain, base,
           coarse_gain, c0, c1, coarse_base, *rest):
    counts = len(STAGES) * len(SIDES)
    send_bufs, recv_bufs = rest[:counts], rest[counts : 2 * counts]
    held = rest[2 * counts : 2 * counts + len(STAGES)]
    load_sem, send_sem, recv_sem, hop_sems = rest[2 * counts + len(STAGES) :]
    band, lane = lax.axis_index("band"), lax.axis_index("lane")
    bands, lanes = lax.axis_size("band"), lax.axis_size("lane")

    loads = [
        pltpu.make_async_copy(src, dst, load_sem.at[i])
        for i, (src, dst) in enumerate(
            ((mass_hbm, mass), (source_hbm, source), (values_hbm, start))
        )
    ]
    for copy in loads:
        copy.start()

    exists, targets = [], []
    for sy, sx in SIDES:
        y, x = band + sy, lane + sx
        exists.append((y >= 0) & (y < bands) & (x >= 0) & (x < lanes))
        targets.append({"band": y, "lane": x})

    barrier = pltpu.get_barrier_semaphore()
    for there, target in zip(exists, targets):

        @pl.when(there)
        def _():
            pl.semaphore_signal(barrier, inc=1, device_id=target, device_id_type=MESH)

    for far, side, between in SLOW:
        other = far + (1 if side else -1)

        @pl.when(lane == between)
        def _():
            pl.semaphore_signal(barrier, inc=1, device_id={"lane": jnp.int32(far)}, device_id_type=MESH)

        @pl.when(lane == other)
        def _():
            pl.semaphore_signal(barrier, inc=1, device_id={"lane": jnp.int32(between)}, device_id_type=MESH)

    for k in range(4):

        @pl.when(jnp.logical_not(exists[k]))
        def _():
            for ref, grid, depth in (
                (u0, FINE, DU), (gain, FINE, DW), (base, FINE, DW),
                (coarse_gain, COARSE, DM), (coarse_base, COARSE, DC),
            ):
                clear(ref, grid, SIDES[k], depth)

    loads[0].wait()

    def coarse_row(y, carry):
        for x in range(0, M, 8):
            total = None
            for dy in range(2):
                for dx in range(2):
                    part = mass[pl.ds((2 * y + dy) * N + 2 * x + dx, 8, stride=2), :]
                    total = part if total is None else total + part
            at = pl.multiple_of(COARSE.at(y, x), 8)
            coarse_gain[pl.ds(at, 8), :] = 0.8 / (4.0 + 0.5 * total)
        return carry

    with jax.named_scope("coarse_setup"):
        lax.fori_loop(0, M, coarse_row, 0)
    with jax.named_scope("load"):
        loads[1].wait()
        loads[2].wait()

    def fine_row(y, carry):
        for x in range(0, N, 8):
            here = pl.ds(pl.multiple_of(y * N + x, 8), 8)
            there = pl.ds(pl.multiple_of(FINE.at(y, x), 8), 8)
            factor = 0.8 / (4.0 + mass[here, :])
            gain[there, :] = factor
            base[there, :] = factor * source[here, :]
            u0[there, :] = start[here, :]
        return carry

    with jax.named_scope("fine_setup"):
        lax.fori_loop(0, N, fine_row, 0)

    def copy_of(stage, k, arriving=False):
        at = stage * len(SIDES) + k
        sy, sx = SIDES[k]
        over = at if arriving else stage * len(SIDES) + SIDES.index((-sy, -sx))
        return pltpu.make_async_remote_copy(
            send_bufs[at], recv_bufs[over], send_sem.at[at], recv_sem.at[over],
            device_id=targets[k], device_id_type=MESH,
        )

    hops = [(stage, i) for stage in range(len(STAGES)) for i in range(CHUNKS[stage])]

    def hop(stage, i, source_of, target, lane_to, leg):
        at = hops.index((stage, i))
        return pltpu.make_async_remote_copy(
            source_of, target, hop_sems.at[leg, 0, at], hop_sems.at[leg, 1, at],
            device_id={"lane": jnp.int32(lane_to)}, device_id_type=MESH,
        )

    def hops_of(leg, stage, far, side, between):
        first, chunks = split(stage)
        other = far + (1 if side else -1)
        out = []
        for i, (start, count) in enumerate(chunks):
            here = held[stage].at[pl.ds(start - first, count)]
            if leg == 0:
                sent = send_bufs[stage * len(SIDES) + side].at[pl.ds(start, count)]
                out.append(hop(stage, i, sent, here, between, 0))
            else:
                got = recv_bufs[stage * len(SIDES) + 1 - side].at[pl.ds(start, count)]
                out.append(hop(stage, i, here, got, other, 1))
        return out

    def straight(stage, k, arriving=False):
        at = stage * len(SIDES) + k
        over = at if arriving else at + 1 - 2 * k
        part = pl.ds(0, split(stage)[0])
        return pltpu.make_async_remote_copy(
            send_bufs[at].at[part], recv_bufs[over].at[part], send_sem.at[at], recv_sem.at[over],
            device_id=targets[k], device_id_type=MESH,
        )

    slow = [lane == far for far, _, _ in SLOW]
    slow_side = {side: i for i, (_, side, _) in enumerate(SLOW)}
    whole = [
        there & jnp.logical_not(slow[slow_side[k]]) if k in slow_side else there
        for k, there in enumerate(exists)
    ]

    def send(stage, refs, among=None):
        among = lane >= 0 if among is None else among
        for k in (1, 0, 4, 5, 6, 7, 2, 3):

            @pl.when(exists[k] & among)
            def _():
                pack(send_bufs[stage * len(SIDES) + k], refs, STAGES[stage], SIDES[k])

            if k in slow_side:

                @pl.when(slow[slow_side[k]] & among)
                def _():
                    for first in hops_of(0, stage, *SLOW[slow_side[k]]):
                        first.start()
                    straight(stage, k).start()

            @pl.when(whole[k] & among)
            def _():
                copy_of(stage, k).start()

    def pass_on(stage):
        for entry in SLOW:

            @pl.when(lane == entry[2])
            def _():
                for first, second in zip(hops_of(0, stage, *entry), hops_of(1, stage, *entry)):
                    first.wait_recv()
                    second.start()

    def receive(stage, refs):
        for k in (2, 3, 4, 5, 6, 7, 0, 1):
            if k in slow_side:

                @pl.when(slow[slow_side[k]])
                def _():
                    straight(stage, k, arriving=True).wait_recv()
                    for second in hops_of(1, stage, *SLOW[1 - slow_side[k]]):
                        second.wait_recv()

            @pl.when(whole[k])
            def _():
                copy_of(stage, k, arriving=True).wait_recv()

            @pl.when(exists[k])
            def _():
                unpack(recv_bufs[stage * len(SIDES) + k], refs, STAGES[stage], SIDES[k])

    total = jnp.int32(0)
    for there in exists:
        total = total + there.astype(jnp.int32)
    for far, _, between in SLOW:
        total = total + (lane == far).astype(jnp.int32) + (lane == between).astype(jnp.int32)
    with jax.named_scope("barrier"):
        pl.semaphore_wait(barrier, total)

    with jax.named_scope("send_a"):
        send(0, (u0, gain, base))
    hurried = slow[0] | slow[1]
    with jax.named_scope("send_m"):
        send(1, (coarse_gain,), hurried)

    wide = ((-DU, 9),)

    def restrict(low, high, groups):
        def restrict_row(y, carry):
            for x in groups:

                def u_at(dy, dx):
                    return u3[pl.ds(FINE.at(2 * y + dy, 2 * x + dx), 8, stride=2), :]

                def own(ref, dy, dx):
                    return ref[pl.ds((2 * y + dy) * N + 2 * x + dx, 8, stride=2), :]

                block = {}
                for dy in range(2):
                    for dx in range(2):
                        block[dy, dx] = u_at(dy, dx)
                total = None
                for dy in range(2):
                    for dx in range(2):
                        here = block[dy, dx]
                        around = (
                            u_at(dy, -1 if dx == 0 else 2) + u_at(-1 if dy == 0 else 2, dx)
                        ) + (block[dy, 1 - dx] + block[1 - dy, dx])
                        defect = (own(source, dy, dx) + around) - (4.0 + own(mass, dy, dx)) * here
                        total = defect if total is None else total + defect
                at = pl.multiple_of(COARSE.at(y, x), 8)
                coarse_base[pl.ds(at, 8), :] = coarse_gain[pl.ds(at, 8), :] * (0.5 * total)
            return carry

        lax.fori_loop(low, high, restrict_row, 0)

    with jax.named_scope("inside"):
        sweep(FINE, u0, u1, gain, base, wide, 1, N - 1)
        sweep(FINE, u1, u2, gain, base, wide, 2, N - 2)
        sweep(FINE, u2, u3, gain, base, wide, 3, N - 3)
        restrict(RIM, M - RIM, range(0, M, 8))
    with jax.named_scope("send_e"):
        send(2, (coarse_base,), hurried)
    with jax.named_scope("pass_a"):
        pass_on(0)
    with jax.named_scope("receive_a"):
        receive(0, (u0, gain, base))
    with jax.named_scope("send_me"):
        send(1, (coarse_gain,), jnp.logical_not(hurried))
        send(2, (coarse_base,), jnp.logical_not(hurried))
    with jax.named_scope("rim"):
        for step, (src, dst) in enumerate(((u0, u1), (u1, u2), (u2, u3))):
            for at in (step - 3, N - 1 - step):
                sweep(FINE, src, dst, gain, base, wide, at, at + 4)
                sweep_strip(FINE, src, dst, gain, base, at, 4)
        restrict(0, RIM, range(0, M, 8))
        restrict(M - RIM, M, range(0, M, 8))
        restrict(RIM, M - RIM, (0, M - 8))
    with jax.named_scope("send_l"):
        send(3, (coarse_base,))
        send(4, (u3,))
    with jax.named_scope("pass_me"):
        pass_on(1)
        pass_on(2)
    with jax.named_scope("receive_m"):
        receive(1, (coarse_gain,))
    with jax.named_scope("receive_e"):
        receive(2, (coarse_base,))
    with jax.named_scope("receive_l"):
        receive(3, (coarse_base,))

    with jax.named_scope("coarse"):
        src, dst = coarse_base, c0
        for step in range(1, INNER):
            depth = DC - step
            span = M + 2 * depth
            if span > 56:
                groups = ((-depth, 4), (-depth + 32, 4))
            else:
                groups = ((-depth, -(-span // 8)),)
            sweep(COARSE, src, dst, coarse_gain, coarse_base, groups, -depth, M + depth)
            src, dst = dst, (c1 if dst is c0 else c0)
    coarse = src

    for k in range(4):

        @pl.when(jnp.logical_not(exists[k]))
        def _():
            clear(u3, FINE, SIDES[k], DV)

    with jax.named_scope("receive_v"):
        receive(4, (u3,))

    def prolong_row(i, carry):
        y = i - 2
        for x in (-2, 6, 14, 22, M - 6):
            add = coarse[pl.ds(COARSE.at(y, x), 8), :]
            for dy in range(2):
                for dx in range(2):
                    at = pl.ds(FINE.at(2 * y + dy, 2 * x + dx), 8, stride=2)
                    u0[at, :] = u3[at, :] + add
        return carry

    with jax.named_scope("prolong"):
        lax.fori_loop(0, M + 4, prolong_row, 0)
    with jax.named_scope("after"):
        sweep(FINE, u0, u1, gain, base, wide, -2, N + 2)
        sweep(FINE, u1, u0, gain, base, wide, -1, N + 1)
        sweep(FINE, u0, out_ref, gain, base, ((0, 4), (32, 4)), 0, N, store_at=lambda y, x: y * N + x)

    for stage in range(len(STAGES)):
        for k in range(len(SIDES)):

            if k in slow_side:

                @pl.when(slow[slow_side[k]])
                def _():
                    for first in hops_of(0, stage, *SLOW[slow_side[k]]):
                        first.wait_send()
                    straight(stage, k).wait_send()

            @pl.when(whole[k])
            def _():
                copy_of(stage, k).wait_send()

        for entry in SLOW:

            @pl.when(lane == entry[2])
            def _():
                for second in hops_of(1, stage, *entry):
                    second.wait_send()


def per_device(source_terms, initial_values, absorption):
    shape = source_terms.shape
    flat = [
        pltpu.with_memory_space_constraint(x.reshape(N * N, CASES), pltpu.HBM)
        for x in (source_terms, initial_values, absorption)
    ]
    vmem = lambda count: pltpu.VMEM((count, CASES), jnp.float32)
    buffers = [vmem(message_rows(parts, side)) for parts in STAGES for side in SIDES]
    result = pl.pallas_call(
        kernel,
        out_shape=pltpu.VMEM((N * N, CASES), jnp.float32),
        in_specs=[pl.BlockSpec(memory_space=pltpu.HBM)] * 3,
        out_specs=pl.BlockSpec(memory_space=pltpu.VMEM),
        scratch_shapes=[vmem(N * N)] * 3
        + [vmem(SIZE_F)] * 6
        + [vmem(SIZE_C)] * 4
        + buffers
        + buffers
        + [vmem(8 + sum(count for _, count in split(stage)[1])) for stage in range(len(STAGES))]
        + [
            pltpu.SemaphoreType.DMA((3,)),
            pltpu.SemaphoreType.DMA((len(buffers),)),
            pltpu.SemaphoreType.DMA((len(buffers),)),
            pltpu.SemaphoreType.DMA((2, 2, sum(CHUNKS))),
        ],
        compiler_params=pltpu.CompilerParams(
            collective_id=0, has_side_effects=True, vmem_limit_bytes=48 << 20
        ),
        name="cycle",
    )(*flat)
    return result.reshape(shape)


def solution(mesh):
    placed = P(("shift", "band"), "lane", None)
    return jax.shard_map(
        per_device,
        mesh=mesh,
        in_specs=(placed,) * 3,
        out_specs=placed,
        check_vma=False,
    )
```

```python
import jax
import jax.numpy as jnp
from jax import lax
from jax.experimental import pallas as pl
from jax.experimental.pallas import tpu as pltpu
from jax.sharding import PartitionSpec as P

CASES = 128
BEFORE = 3
AFTER = 3
INNER = 13
N = 64
M = N // 2
DU = BEFORE + 1
DW = BEFORE
DV = AFTER
DC = INNER + 1
DM = INNER

PF, YF, XF = 88, 4, 8
SIZE_F = (N + 2 * YF) * PF
PC, YC, XC = 72, 14, 16
SIZE_C = (M + 2 * YC) * PC

SLOW = ((7, 1, 8, (4, 6, 5)), (8, 0, 7, (11, 9, 10)))
CHUNKS = (
    ((96, 96), (88, 88), (72, 72)),
    ((136,), (128,), (112,)),
    ((104,), (104,), (88,)),
    ((), (), ()),
    ((), (), ()),
    ((), (), ()),
    ((), (), ()),
)
SIDES = ((0, -1), (0, 1), (-1, 0), (1, 0), (-1, -1), (-1, 1), (1, -1), (1, 1))
MESH = pl.DeviceIdType.MESH


def split(stage):
    first = message_rows(STAGES[stage], (0, 1)) - sum(sum(route) for route in CHUNKS[stage])
    at, routes = first, []
    for route in CHUNKS[stage]:
        routes.append([])
        for count in route:
            routes[-1].append((at, count))
            at += count
    return first, routes


HOPS = [
    (stage, route, chunk)
    for stage in range(len(CHUNKS))
    for route in range(len(CHUNKS[stage]))
    for chunk in range(len(CHUNKS[stage][route]))
]


class Grid:
    def __init__(self, size, pitch, y_off, x_off):
        self.size, self.pitch, self.y_off, self.x_off = size, pitch, y_off, x_off

    def at(self, y, x):
        return (y + self.y_off) * self.pitch + x + self.x_off


FINE = Grid(N, PF, YF, XF)
COARSE = Grid(M, PC, YC, XC)


def runs(grid, side, boxes, sending):
    def place(sign, low, high, own):
        n = grid.size
        if sign == 0:
            return low, high - low
        if own:
            return (n - high if sign > 0 else low - 1), high - low + 1
        return (n - 1 + low if sign > 0 else -high), high - low + 1

    out = []
    for y_range, x_range, along_x in boxes:
        y, height = place(side[0], *y_range, sending[0])
        x, width = place(side[1], *x_range, sending[1])
        if along_x:
            out += [(grid.at(y + i, x), width, 1) for i in range(height)]
        else:
            out += [(grid.at(y, x + i), height, grid.pitch) for i in range(width)]
    return out


def whole_halo(grid, side, depth):
    own = (0, grid.size)
    if side[0] == 0:
        return [(own, (1, depth), False)]
    if side[1] == 0:
        return [((1, depth), own, True)]
    return [((1, depth - dx), (dx, dx), False) for dx in range(1, depth)]


RIM = 2


def early_halo(grid, side, depth):
    own, deep = (RIM, grid.size - RIM), (RIM + 1, depth)
    if side[0] == 0:
        return [(own, deep, False)]
    if side[1] == 0:
        return [(deep, own, True)]
    return [((RIM + 1, depth - dx), (dx, dx), False) for dx in range(RIM + 1, depth - RIM)]


def late_halo(grid, side, depth):
    n = grid.size
    own, near, deep = (0, n), (1, RIM), (RIM + 1, depth)
    ends = [(0, RIM), (n - RIM, n)]
    if side[0] == 0:
        return [(own, near, False)] + [(end, deep, True) for end in ends]
    if side[1] == 0:
        return [(near, own, True)] + [(deep, end, False) for end in ends]
    return [((1, depth - dx), (dx, dx), False) for dx in range(1, RIM + 1)] + [
        ((dy, dy), (RIM + 1, depth - dy), True) for dy in range(1, RIM + 1)
    ]


def far_halo(grid, side, depth):
    own = (0, grid.size)
    if side[0] == 0:
        return [(own, (2, depth), False)]
    if side[1] == 0:
        return [((2, depth), own, True)]
    return whole_halo(grid, side, depth)


def pieces(part, side, sending):
    grid, depth, boxes, corners = part
    if not corners:
        return runs(grid, side, boxes(grid, side, depth), (sending, sending))
    both = [(sy, side[1]) for sy in (-1, 1)]
    return [
        run
        for corner in both
        for run in runs(grid, corner, boxes(grid, corner, depth), (False, sending))
    ]


def message_rows(parts, side):
    total = sum(
        count for part in parts for _, count, _ in pieces(part, side, True)
    )
    return -(-total // 8) * 8


def rows(start, count, stride):
    return pl.ds(start, count) if stride == 1 else pl.ds(start, count, stride=stride)


def pack(buffer, refs, parts, side):
    at = 0
    for ref, part in zip(refs, parts):
        for start, count, stride in pieces(part, side, True):
            buffer[pl.ds(at, count), :] = ref[rows(start, count, stride), :]
            at += count


def unpack(buffer, refs, parts, side):
    at = 0
    for ref, part in zip(refs, parts):
        for start, count, stride in pieces(part, side, False):
            ref[rows(start, count, stride), :] = buffer[pl.ds(at, count), :]
            at += count


def clear(ref, grid, side, depth):
    sy, sx = side
    n = grid.size
    if sy == 0:
        for i in range(depth):
            x = n + i if sx > 0 else -1 - i
            count = n + 2 * grid.y_off
            ref[pl.ds(grid.at(-grid.y_off, x), count, stride=grid.pitch), :] = jnp.zeros(
                (count, CASES), jnp.float32
            )
    else:
        y0 = n if sy > 0 else -depth
        count = depth * grid.pitch
        ref[pl.ds(grid.at(y0, -grid.x_off), count), :] = jnp.zeros((count, CASES), jnp.float32)


STAGES = (
    tuple((FINE, depth, whole_halo, False) for depth in (DU, DW, DW)),
    ((COARSE, DM, whole_halo, False),),
    ((COARSE, DC, early_halo, False),),
    ((COARSE, DC, late_halo, False),),
    ((FINE, DV, far_halo, False),),
    ((COARSE, DM, whole_halo, True),),
    ((COARSE, DC, early_halo, True),),
)
ALL = (1, 0, 2, 3, 4, 5, 6, 7)
STAGE_SIDES = (ALL, ALL, ALL, ALL, ALL, ALL[:2], ALL[:2])
CORNERS_BY_SIDES = (1, 2)


def sweep(grid, src, dst, gain, base, groups, y_low, y_high, store_at=None, unroll=4):
    store_at = store_at or grid.at
    blocks = -(-(y_high - y_low) // unroll)

    def block(i, carry):
        y = jnp.minimum(y_low + i * unroll, y_high - unroll)
        row = grid.at(y, 0)
        out_row = store_at(y, 0)
        out_pitch = store_at(1, 0) - store_at(0, 0)
        for x0, width in groups:

            def load(ref, dy, x):
                return ref[pl.ds(row + dy * grid.pitch + x0 + x, 8, stride=width), :]

            left = [load(src, k, -1) for k in range(unroll)]
            here = [load(src, k, 0) for k in range(unroll)]
            for x in range(width):
                right = [load(src, k, x + 1) for k in range(unroll)]
                above = load(src, -1, x)
                below = load(src, unroll, x)
                for k in range(unroll):
                    up = here[k - 1] if k else above
                    down = here[k + 1] if k + 1 < unroll else below
                    around = (left[k] + right[k]) + (up + down)
                    new = (
                        0.2 * here[k] + load(base, k, x) + load(gain, k, x) * around
                    )
                    dst[pl.ds(out_row + k * out_pitch + x0 + x, 8, stride=width), :] = new
                left, here = here, right
        return carry

    lax.fori_loop(0, blocks, block, 0)


def sweep_strip(grid, src, dst, gain, base, x0, width):
    def block(i, carry):
        row = grid.at(8 * i, x0)

        def load(ref, dy, x):
            return ref[pl.ds(row + dy * grid.pitch + x, 8, stride=grid.pitch), :]

        left, here = load(src, 0, -1), load(src, 0, 0)
        for x in range(width):
            right = load(src, 0, x + 1)
            around = (left + right) + (load(src, -1, x) + load(src, 1, x))
            new = 0.2 * here + load(base, 0, x) + load(gain, 0, x) * around
            dst[pl.ds(row + x, 8, stride=grid.pitch), :] = new
            left, here = here, right
        return carry

    lax.fori_loop(0, grid.size // 8, block, 0)


def kernel(source_hbm, values_hbm, mass_hbm, out_ref, source, start, mass, u0, u1, u2, u3, gain, base,
           coarse_gain, c0, c1, coarse_base, *rest):
    counts = len(STAGES) * len(SIDES)
    send_bufs, recv_bufs = rest[:counts], rest[counts : 2 * counts]
    held = rest[2 * counts : 2 * counts + len(STAGES)]
    load_sem, send_sem, recv_sem, hop_sems = rest[2 * counts + len(STAGES) :]
    band, lane = lax.axis_index("band"), lax.axis_index("lane")
    bands, lanes = lax.axis_size("band"), lax.axis_size("lane")

    loads = [
        pltpu.make_async_copy(src, dst, load_sem.at[i])
        for i, (src, dst) in enumerate(
            ((mass_hbm, mass), (source_hbm, source), (values_hbm, start))
        )
    ]
    for copy in loads:
        copy.start()

    exists, targets = [], []
    for sy, sx in SIDES:
        y, x = band + sy, lane + sx
        exists.append((y >= 0) & (y < bands) & (x >= 0) & (x < lanes))
        targets.append({"band": y, "lane": x})

    barrier = pltpu.get_barrier_semaphore()
    for there, target in zip(exists, targets):

        @pl.when(there)
        def _():
            pl.semaphore_signal(barrier, inc=1, device_id=target, device_id_type=MESH)

    def tell(lane_to):
        pl.semaphore_signal(
            barrier, inc=1, device_id={"lane": jnp.int32(lane_to)}, device_id_type=MESH
        )

    for far, _, _, betweens in SLOW:
        for between in betweens:

            @pl.when(lane == between)
            def _():
                tell(far)

    for k in range(4):

        @pl.when(jnp.logical_not(exists[k]))
        def _():
            for ref, grid, depth in (
                (u0, FINE, DU), (gain, FINE, DW), (base, FINE, DW),
                (coarse_gain, COARSE, DM), (coarse_base, COARSE, DC),
            ):
                clear(ref, grid, SIDES[k], depth)

    loads[0].wait()

    def coarse_row(y, carry):
        for x in range(0, M, 8):
            total = None
            for dy in range(2):
                for dx in range(2):
                    part = mass[pl.ds((2 * y + dy) * N + 2 * x + dx, 8, stride=2), :]
                    total = part if total is None else total + part
            at = pl.multiple_of(COARSE.at(y, x), 8)
            coarse_gain[pl.ds(at, 8), :] = 0.8 / (4.0 + 0.5 * total)
        return carry

    with jax.named_scope("coarse_setup"):
        lax.fori_loop(0, M, coarse_row, 0)
    with jax.named_scope("load"):
        loads[1].wait()
        loads[2].wait()

    def fine_row(y, carry):
        for x in range(0, N, 8):
            here = pl.ds(pl.multiple_of(y * N + x, 8), 8)
            there = pl.ds(pl.multiple_of(FINE.at(y, x), 8), 8)
            factor = 0.8 / (4.0 + mass[here, :])
            gain[there, :] = factor
            base[there, :] = factor * source[here, :]
            u0[there, :] = start[here, :]
        return carry

    with jax.named_scope("fine_setup"):
        lax.fori_loop(0, N, fine_row, 0)

    def copy_of(stage, k, arriving=False):
        at = stage * len(SIDES) + k
        sy, sx = SIDES[k]
        over = at if arriving else stage * len(SIDES) + SIDES.index((-sy, -sx))
        return pltpu.make_async_remote_copy(
            send_bufs[at], recv_bufs[over], send_sem.at[at], recv_sem.at[over],
            device_id=targets[k], device_id_type=MESH,
        )

    def hops_of(leg, stage, entry, route):
        _, side, other, betweens = entry
        chunks = split(stage)[1][route]
        out = []
        for i, (start, count) in enumerate(chunks):
            at = HOPS.index((stage, route, i))
            here = held[stage].at[pl.ds(start - chunks[0][0], count)]
            if leg == 0:
                source = send_bufs[stage * len(SIDES) + side].at[pl.ds(start, count)]
                target, lane_to = here, betweens[route]
            else:
                source, lane_to = here, other
                target = recv_bufs[stage * len(SIDES) + 1 - side].at[pl.ds(start, count)]
            out.append(
                pltpu.make_async_remote_copy(
                    source, target, hop_sems.at[leg, 0, at], hop_sems.at[leg, 1, at],
                    device_id={"lane": jnp.int32(lane_to)}, device_id_type=MESH,
                )
            )
        return out

    def all_hops(leg, stage, entry):
        per_route = [hops_of(leg, stage, entry, route) for route in range(len(entry[3]))]
        return [copy for copies in per_route for copy in copies]

    def straight(stage, k, arriving=False):
        at = stage * len(SIDES) + k
        over = at if arriving else at + 1 - 2 * k
        part = pl.ds(0, split(stage)[0])
        return pltpu.make_async_remote_copy(
            send_bufs[at].at[part], recv_bufs[over].at[part], send_sem.at[at], recv_sem.at[over],
            device_id=targets[k], device_id_type=MESH,
        )

    slow = [lane == entry[0] for entry in SLOW]
    slow_side = {entry[1]: i for i, entry in enumerate(SLOW)}
    whole = [
        there & jnp.logical_not(slow[slow_side[k]]) if k in slow_side else there
        for k, there in enumerate(exists)
    ]

    def crosses(k):
        for i, entry in enumerate(SLOW):
            if SIDES[k][1] == entry[2] - entry[0]:
                return slow[i]
        return None

    def in_one(stage, k):
        if k in slow_side:
            return whole[k]
        if stage in CORNERS_BY_SIDES and k >= 4:
            return exists[k] & crosses(k)
        return exists[k]

    def in_parts(stage, k):
        if k not in slow_side or any(corners for _, _, _, corners in STAGES[stage]):
            return None
        return slow[slow_side[k]]

    def send_across(stage, refs):
        for k in STAGE_SIDES[stage]:
            if crosses(k) is None:
                continue

            @pl.when(exists[k] & crosses(k))
            def _():
                pack(send_bufs[stage * len(SIDES) + k], refs, STAGES[stage], SIDES[k])
                if k in slow_side:
                    for copy in all_hops(0, stage, SLOW[slow_side[k]]):
                        copy.start()
                    straight(stage, k).start()
                else:
                    copy_of(stage, k).start()

    relays = jnp.bool_(False)
    for entry in SLOW:
        for between in entry[3]:
            relays = relays | (lane == between)

    def send(stage, refs, sides=None, among=None):
        for k in STAGE_SIDES[stage] if sides is None else sides:
            there = exists[k] if among is None else exists[k] & among
            if crosses(k) is not None:
                there = there & jnp.logical_not(crosses(k))

            @pl.when(there)
            def _():
                pack(send_bufs[stage * len(SIDES) + k], refs, STAGES[stage], SIDES[k])
                copy_of(stage, k).start()

    def pass_on(stage):
        for entry in SLOW:
            for route, between in enumerate(entry[3]):
                if CHUNKS[stage][route]:

                    @pl.when(lane == between)
                    def _():
                        for first, second in zip(
                            hops_of(0, stage, entry, route), hops_of(1, stage, entry, route)
                        ):
                            first.wait_recv()
                            second.start()

    def receive(stage, refs, sides=(2, 3, 4, 5, 6, 7, 0, 1)):
        for k in sides:
            if k not in STAGE_SIDES[stage]:
                continue

            @pl.when(in_one(stage, k))
            def _():
                copy_of(stage, k, arriving=True).wait_recv()
                if in_parts(stage, k) is None:
                    unpack(recv_bufs[stage * len(SIDES) + k], refs, STAGES[stage], SIDES[k])

            if in_parts(stage, k) is not None:

                @pl.when(in_parts(stage, k))
                def _():
                    straight(stage, k, arriving=True).wait_recv()
                    for copy in all_hops(1, stage, SLOW[1 - slow_side[k]]):
                        copy.wait_recv()

                @pl.when(exists[k])
                def _():
                    unpack(recv_bufs[stage * len(SIDES) + k], refs, STAGES[stage], SIDES[k])

    total = jnp.int32(0)
    for there in exists:
        total = total + there.astype(jnp.int32)
    for far, _, _, betweens in SLOW:
        total = total + (lane == far).astype(jnp.int32) * len(betweens)
    with jax.named_scope("barrier"):
        pl.semaphore_wait(barrier, total)

    with jax.named_scope("cross_am"):
        send_across(0, (u0, gain, base))
        send_across(1, (coarse_gain,))
    with jax.named_scope("send_a"):
        send(0, (u0, gain, base), (1, 0, 4, 5, 6, 7))
        send(0, (u0, gain, base), (2, 3), jnp.logical_not(relays))

    wide = ((-DU, 9),)

    def restrict(low, high, groups):
        def restrict_row(y, carry):
            for x in groups:

                def u_at(dy, dx):
                    return u3[pl.ds(FINE.at(2 * y + dy, 2 * x + dx), 8, stride=2), :]

                def own(ref, dy, dx):
                    return ref[pl.ds((2 * y + dy) * N + 2 * x + dx, 8, stride=2), :]

                block = {}
                for dy in range(2):
                    for dx in range(2):
                        block[dy, dx] = u_at(dy, dx)
                total = None
                for dy in range(2):
                    for dx in range(2):
                        here = block[dy, dx]
                        around = (
                            u_at(dy, -1 if dx == 0 else 2) + u_at(-1 if dy == 0 else 2, dx)
                        ) + (block[dy, 1 - dx] + block[1 - dy, dx])
                        defect = (own(source, dy, dx) + around) - (4.0 + own(mass, dy, dx)) * here
                        total = defect if total is None else total + defect
                at = pl.multiple_of(COARSE.at(y, x), 8)
                coarse_base[pl.ds(at, 8), :] = coarse_gain[pl.ds(at, 8), :] * (0.5 * total)
            return carry

        lax.fori_loop(low, high, restrict_row, 0)

    with jax.named_scope("inside"):
        sweep(FINE, u0, u1, gain, base, wide, 1, N - 1)
        sweep(FINE, u1, u2, gain, base, wide, 2, N - 2)
        sweep(FINE, u2, u3, gain, base, wide, 3, N - 3)
        restrict(RIM, M - RIM, range(0, M, 8))
    with jax.named_scope("cross_e"):
        send_across(2, (coarse_base,))
    with jax.named_scope("pass_a"):
        pass_on(0)
    with jax.named_scope("send_a_late"):
        send(0, (u0, gain, base), (2, 3), relays)
    with jax.named_scope("pass_m"):
        pass_on(1)
    with jax.named_scope("pass_e"):
        pass_on(2)
    with jax.named_scope("receive_a"):
        receive(0, (u0, gain, base))
    with jax.named_scope("send_me"):
        send(1, (coarse_gain,), ALL[:4])
        send(2, (coarse_base,), ALL[:4])
    with jax.named_scope("rim"):
        for step, (src, dst) in enumerate(((u0, u1), (u1, u2), (u2, u3))):
            for at in (step - 3, N - 1 - step):
                sweep(FINE, src, dst, gain, base, wide, at, at + 4)
                sweep_strip(FINE, src, dst, gain, base, at, 4)
        restrict(0, RIM, range(0, M, 8))
        restrict(M - RIM, M, range(0, M, 8))
        restrict(RIM, M - RIM, (0, M - 8))
    with jax.named_scope("send_l"):
        send_across(3, (coarse_base,))
        send(3, (coarse_base,))
        send_across(4, (u3,))
        send(4, (u3,))
    with jax.named_scope("receive_my"):
        receive(1, (coarse_gain,), (2, 3))
        send(5, (coarse_gain,))
    with jax.named_scope("receive_ey"):
        receive(2, (coarse_base,), (2, 3))
        send(6, (coarse_base,))
    with jax.named_scope("receive_m"):
        receive(1, (coarse_gain,), (4, 5, 6, 7, 0, 1))
        receive(5, (coarse_gain,))
    with jax.named_scope("receive_e"):
        receive(2, (coarse_base,), (4, 5, 6, 7, 0, 1))
        receive(6, (coarse_base,))
    with jax.named_scope("receive_l"):
        receive(3, (coarse_base,))

    with jax.named_scope("coarse"):
        src, dst = coarse_base, c0
        for step in range(1, INNER):
            depth = DC - step
            span = M + 2 * depth
            if span > 56:
                groups = ((-depth, 4), (-depth + 32, 4))
            else:
                groups = ((-depth, -(-span // 8)),)
            sweep(COARSE, src, dst, coarse_gain, coarse_base, groups, -depth, M + depth)
            src, dst = dst, (c1 if dst is c0 else c0)
    coarse = src

    for k in range(4):

        @pl.when(jnp.logical_not(exists[k]))
        def _():
            clear(u3, FINE, SIDES[k], DV)

    with jax.named_scope("receive_v"):
        receive(4, (u3,))

    def prolong_row(i, carry):
        y = i - 2
        for x in (-2, 6, 14, 22, M - 6):
            add = coarse[pl.ds(COARSE.at(y, x), 8), :]
            for dy in range(2):
                for dx in range(2):
                    at = pl.ds(FINE.at(2 * y + dy, 2 * x + dx), 8, stride=2)
                    u0[at, :] = u3[at, :] + add
        return carry

    with jax.named_scope("prolong"):
        lax.fori_loop(0, M + 4, prolong_row, 0)
    with jax.named_scope("after"):
        sweep(FINE, u0, u1, gain, base, wide, -2, N + 2)
        sweep(FINE, u1, u0, gain, base, wide, -1, N + 1)
        sweep(FINE, u0, out_ref, gain, base, ((0, 4), (32, 4)), 0, N, store_at=lambda y, x: y * N + x)

    for stage in range(len(STAGES)):
        for k in STAGE_SIDES[stage]:

            if in_parts(stage, k) is not None:

                @pl.when(in_parts(stage, k))
                def _():
                    for copy in all_hops(0, stage, SLOW[slow_side[k]]):
                        copy.wait_send()
                    straight(stage, k).wait_send()

            @pl.when(in_one(stage, k))
            def _():
                copy_of(stage, k).wait_send()

        for entry in SLOW:
            for route, between in enumerate(entry[3]):
                if CHUNKS[stage][route]:

                    @pl.when(lane == between)
                    def _():
                        for copy in hops_of(1, stage, entry, route):
                            copy.wait_send()


def per_device(source_terms, initial_values, absorption):
    shape = source_terms.shape
    flat = [
        pltpu.with_memory_space_constraint(x.reshape(N * N, CASES), pltpu.HBM)
        for x in (source_terms, initial_values, absorption)
    ]
    vmem = lambda count: pltpu.VMEM((count, CASES), jnp.float32)
    buffers = [
        vmem(message_rows(parts, side) if k in sides else 8)
        for parts, sides in zip(STAGES, STAGE_SIDES)
        for k, side in enumerate(SIDES)
    ]
    result = pl.pallas_call(
        kernel,
        out_shape=pltpu.VMEM((N * N, CASES), jnp.float32),
        in_specs=[pl.BlockSpec(memory_space=pltpu.HBM)] * 3,
        out_specs=pl.BlockSpec(memory_space=pltpu.VMEM),
        scratch_shapes=[vmem(N * N)] * 3
        + [vmem(SIZE_F)] * 6
        + [vmem(SIZE_C)] * 4
        + buffers
        + buffers
        + [vmem(max(8, *(sum(route) for route in routes))) for routes in CHUNKS]
        + [
            pltpu.SemaphoreType.DMA((3,)),
            pltpu.SemaphoreType.DMA((len(buffers),)),
            pltpu.SemaphoreType.DMA((len(buffers),)),
            pltpu.SemaphoreType.DMA((2, 2, len(HOPS))),
        ],
        compiler_params=pltpu.CompilerParams(
            collective_id=0, has_side_effects=True, vmem_limit_bytes=48 << 20
        ),
        name="cycle",
    )(*flat)
    return result.reshape(shape)


def solution(mesh):
    placed = P(("shift", "band"), "lane", None)
    return jax.shard_map(
        per_device,
        mesh=mesh,
        in_specs=(placed,) * 3,
        out_specs=placed,
        check_vma=False,
    )
```

```python
import jax
import jax.numpy as jnp
from jax import lax
from jax.experimental import pallas as pl
from jax.experimental.pallas import tpu as pltpu
from jax.sharding import PartitionSpec as P

CASES = 128
BEFORE = 3
AFTER = 3
INNER = 13
N = 64
M = N // 2
DU = BEFORE + 1
DW = BEFORE
DV = AFTER
DC = INNER + 1
DM = INNER

PF, YF, XF = 88, 4, 8
SIZE_F = (N + 2 * YF) * PF
PC, YC, XC = 72, 14, 16
SIZE_C = (M + 2 * YC) * PC

SLOW = ((7, 1, 8, (4, 6, 5)), (8, 0, 7, (11, 9, 10)))
CHUNKS = (
    ((96, 96), (88, 88), (72, 72)),
    ((136,), (128,), (112,)),
    ((104,), (104,), (88,)),
    ((), (), ()),
    ((), (), ()),
    ((), (), ()),
    ((), (), ()),
)
SIDES = ((0, -1), (0, 1), (-1, 0), (1, 0), (-1, -1), (-1, 1), (1, -1), (1, 1))
MESH = pl.DeviceIdType.MESH


def sem_of(stage, k):
    return SEMS.index(sem_key(stage, k))


def sem_key(stage, k):
    if stage in CORNERS_BY_SIDES and k >= 4:
        return stage, "corner", SIDES[k][0]
    return stage, "side", k


def split(stage):
    first = message_rows(STAGES[stage], (0, 1)) - sum(sum(route) for route in CHUNKS[stage])
    at, routes = first, []
    for route in CHUNKS[stage]:
        routes.append([])
        for count in route:
            routes[-1].append((at, count))
            at += count
    return first, routes


HOPS = [
    (stage, route, chunk)
    for stage in range(len(CHUNKS))
    for route in range(len(CHUNKS[stage]))
    for chunk in range(len(CHUNKS[stage][route]))
]


class Grid:
    def __init__(self, size, pitch, y_off, x_off):
        self.size, self.pitch, self.y_off, self.x_off = size, pitch, y_off, x_off

    def at(self, y, x):
        return (y + self.y_off) * self.pitch + x + self.x_off


FINE = Grid(N, PF, YF, XF)
COARSE = Grid(M, PC, YC, XC)


def runs(grid, side, boxes, sending):
    def place(sign, low, high, own):
        n = grid.size
        if sign == 0:
            return low, high - low
        if own:
            return (n - high if sign > 0 else low - 1), high - low + 1
        return (n - 1 + low if sign > 0 else -high), high - low + 1

    out = []
    for y_range, x_range, along_x in boxes:
        y, height = place(side[0], *y_range, sending[0])
        x, width = place(side[1], *x_range, sending[1])
        if along_x:
            out += [(grid.at(y + i, x), width, 1) for i in range(height)]
        else:
            out += [(grid.at(y, x + i), height, grid.pitch) for i in range(width)]
    return out


def whole_halo(grid, side, depth):
    own = (0, grid.size)
    if side[0] == 0:
        return [(own, (1, depth), False)]
    if side[1] == 0:
        return [((1, depth), own, True)]
    return [((1, depth - dx), (dx, dx), False) for dx in range(1, depth)]


PARTS = 4
RIM = 2


def early_halo(grid, side, depth):
    own, deep = (RIM, grid.size - RIM), (RIM + 1, depth)
    if side[0] == 0:
        return [(own, deep, False)]
    if side[1] == 0:
        return [(deep, own, True)]
    return [((RIM + 1, depth - dx), (dx, dx), False) for dx in range(RIM + 1, depth - RIM)]


def late_halo(grid, side, depth):
    n = grid.size
    own, near, deep = (0, n), (1, RIM), (RIM + 1, depth)
    ends = [(0, RIM), (n - RIM, n)]
    if side[0] == 0:
        return [(own, near, False)] + [(end, deep, True) for end in ends]
    if side[1] == 0:
        return [(near, own, True)] + [(deep, end, False) for end in ends]
    return [((1, depth - dx), (dx, dx), False) for dx in range(1, RIM + 1)] + [
        ((dy, dy), (RIM + 1, depth - dy), True) for dy in range(1, RIM + 1)
    ]


def far_halo(grid, side, depth):
    own = (0, grid.size)
    if side[0] == 0:
        return [(own, (2, depth), False)]
    if side[1] == 0:
        return [((2, depth), own, True)]
    return whole_halo(grid, side, depth)


def pieces(part, side, sending):
    grid, depth, boxes, corners = part
    if not corners:
        return runs(grid, side, boxes(grid, side, depth), (sending, sending))
    both = [(sy, side[1]) for sy in (-1, 1)]
    return [
        run
        for corner in both
        for run in runs(grid, corner, boxes(grid, corner, depth), (False, sending))
    ]


def message_rows(parts, side):
    total = sum(
        count for part in parts for _, count, _ in pieces(part, side, True)
    )
    return -(-total // 8) * 8


def rows(start, count, stride):
    return pl.ds(start, count) if stride == 1 else pl.ds(start, count, stride=stride)


def pack(buffer, refs, parts, side):
    at = 0
    for ref, part in zip(refs, parts):
        for start, count, stride in pieces(part, side, True):
            buffer[pl.ds(at, count), :] = ref[rows(start, count, stride), :]
            at += count


def unpack(buffer, refs, parts, side):
    at = 0
    for ref, part in zip(refs, parts):
        for start, count, stride in pieces(part, side, False):
            ref[rows(start, count, stride), :] = buffer[pl.ds(at, count), :]
            at += count


def clear(ref, grid, side, depth):
    sy, sx = side
    n = grid.size
    if sy == 0:
        for i in range(depth):
            x = n + i if sx > 0 else -1 - i
            count = n + 2 * grid.y_off
            ref[pl.ds(grid.at(-grid.y_off, x), count, stride=grid.pitch), :] = jnp.zeros(
                (count, CASES), jnp.float32
            )
    else:
        y0 = n if sy > 0 else -depth
        count = depth * grid.pitch
        ref[pl.ds(grid.at(y0, -grid.x_off), count), :] = jnp.zeros((count, CASES), jnp.float32)


STAGES = (
    tuple((FINE, depth, whole_halo, False) for depth in (DU, DW, DW)),
    ((COARSE, DM, whole_halo, False),),
    ((COARSE, DC, early_halo, False),),
    ((COARSE, DC, late_halo, False),),
    ((FINE, DV, far_halo, False),),
    ((COARSE, DM, whole_halo, True),),
    ((COARSE, DC, early_halo, True),),
)
ALL = (1, 0, 2, 3, 4, 5, 6, 7)
CORNERS_FIRST = (1, 0, 4, 5, 6, 7, 2, 3)
STAGE_SIDES = (CORNERS_FIRST, ALL, ALL, CORNERS_FIRST, CORNERS_FIRST, ALL[:2], ALL[:2])
CORNERS_BY_SIDES = (1, 2)
SEMS = list(dict.fromkeys(sem_key(stage, k) for stage, ks in enumerate(STAGE_SIDES) for k in ks))


def sweep(grid, src, dst, gain, base, groups, y_low, y_high, store_at=None, unroll=4):
    store_at = store_at or grid.at
    blocks = -(-(y_high - y_low) // unroll)

    def block(i, carry):
        y = jnp.minimum(y_low + i * unroll, y_high - unroll)
        row = grid.at(y, 0)
        out_row = store_at(y, 0)
        out_pitch = store_at(1, 0) - store_at(0, 0)
        for x0, width in groups:

            def load(ref, dy, x):
                return ref[pl.ds(row + dy * grid.pitch + x0 + x, 8, stride=width), :]

            left = [load(src, k, -1) for k in range(unroll)]
            here = [load(src, k, 0) for k in range(unroll)]
            for x in range(width):
                right = [load(src, k, x + 1) for k in range(unroll)]
                above = load(src, -1, x)
                below = load(src, unroll, x)
                for k in range(unroll):
                    up = here[k - 1] if k else above
                    down = here[k + 1] if k + 1 < unroll else below
                    around = (left[k] + right[k]) + (up + down)
                    new = (
                        0.2 * here[k] + load(base, k, x) + load(gain, k, x) * around
                    )
                    dst[pl.ds(out_row + k * out_pitch + x0 + x, 8, stride=width), :] = new
                left, here = here, right
        return carry

    lax.fori_loop(0, blocks, block, 0)


def sweep_strip(grid, src, dst, gain, base, x0, width):
    def block(i, carry):
        row = grid.at(8 * i, x0)

        def load(ref, dy, x):
            return ref[pl.ds(row + dy * grid.pitch + x, 8, stride=grid.pitch), :]

        left, here = load(src, 0, -1), load(src, 0, 0)
        for x in range(width):
            right = load(src, 0, x + 1)
            around = (left + right) + (load(src, -1, x) + load(src, 1, x))
            new = 0.2 * here + load(base, 0, x) + load(gain, 0, x) * around
            dst[pl.ds(row + x, 8, stride=grid.pitch), :] = new
            left, here = here, right
        return carry

    lax.fori_loop(0, grid.size // 8, block, 0)


def kernel(source_hbm, values_hbm, mass_hbm, out_ref, source, start, mass, u0, u1, u2, u3, gain, base,
           coarse_gain, c0, c1, coarse_base, *rest):
    counts = len(STAGES) * len(SIDES)
    send_bufs, recv_bufs = rest[:counts], rest[counts : 2 * counts]
    held = rest[2 * counts : 2 * counts + len(STAGES)]
    load_sem, send_sem, recv_sem, hop_sems, store_sem, result = rest[2 * counts + len(STAGES) :]
    band, lane = lax.axis_index("band"), lax.axis_index("lane")
    bands, lanes = lax.axis_size("band"), lax.axis_size("lane")

    loads = [
        pltpu.make_async_copy(src, dst, load_sem.at[i])
        for i, (src, dst) in enumerate(
            ((mass_hbm, mass), (source_hbm, source), (values_hbm, start))
        )
    ]
    for copy in loads:
        copy.start()

    exists, targets = [], []
    for sy, sx in SIDES:
        y, x = band + sy, lane + sx
        exists.append((y >= 0) & (y < bands) & (x >= 0) & (x < lanes))
        targets.append({"band": y, "lane": x})

    barrier = pltpu.get_barrier_semaphore()
    for there, target in zip(exists, targets):

        @pl.when(there)
        def _():
            pl.semaphore_signal(barrier, inc=1, device_id=target, device_id_type=MESH)

    def tell(lane_to):
        pl.semaphore_signal(
            barrier, inc=1, device_id={"lane": jnp.int32(lane_to)}, device_id_type=MESH
        )

    for far, _, _, betweens in SLOW:
        for between in betweens:

            @pl.when(lane == between)
            def _():
                tell(far)

    for k in range(4):

        @pl.when(jnp.logical_not(exists[k]))
        def _():
            for ref, grid, depth in (
                (u0, FINE, DU), (gain, FINE, DW), (base, FINE, DW),
                (coarse_gain, COARSE, DM), (coarse_base, COARSE, DC),
            ):
                clear(ref, grid, SIDES[k], depth)

    loads[0].wait()

    def coarse_row(y, carry):
        for x in range(0, M, 8):
            total = None
            for dy in range(2):
                for dx in range(2):
                    part = mass[pl.ds((2 * y + dy) * N + 2 * x + dx, 8, stride=2), :]
                    total = part if total is None else total + part
            at = pl.multiple_of(COARSE.at(y, x), 8)
            coarse_gain[pl.ds(at, 8), :] = 0.8 / (4.0 + 0.5 * total)
        return carry

    with jax.named_scope("coarse_setup"):
        lax.fori_loop(0, M, coarse_row, 0)
    with jax.named_scope("load"):
        loads[1].wait()
        loads[2].wait()

    def fine_row(y, carry):
        for x in range(0, N, 8):
            here = pl.ds(pl.multiple_of(y * N + x, 8), 8)
            there = pl.ds(pl.multiple_of(FINE.at(y, x), 8), 8)
            factor = 0.8 / (4.0 + mass[here, :])
            gain[there, :] = factor
            base[there, :] = factor * source[here, :]
            u0[there, :] = start[here, :]
        return carry

    with jax.named_scope("fine_setup"):
        lax.fori_loop(0, N, fine_row, 0)

    def copy_of(stage, k, arriving=False):
        at = stage * len(SIDES) + k
        sy, sx = SIDES[k]
        over = at if arriving else stage * len(SIDES) + SIDES.index((-sy, -sx))
        return pltpu.make_async_remote_copy(
            send_bufs[at], recv_bufs[over],
            send_sem.at[sem_of(stage, k)], recv_sem.at[sem_of(stage, over % len(SIDES))],
            device_id=targets[k], device_id_type=MESH,
        )

    def hops_of(leg, stage, entry, route):
        _, side, other, betweens = entry
        chunks = split(stage)[1][route]
        out = []
        for i, (start, count) in enumerate(chunks):
            at = HOPS.index((stage, route, i))
            here = held[stage].at[pl.ds(start - chunks[0][0], count)]
            if leg == 0:
                source = send_bufs[stage * len(SIDES) + side].at[pl.ds(start, count)]
                target, lane_to = here, betweens[route]
            else:
                source, lane_to = here, other
                target = recv_bufs[stage * len(SIDES) + 1 - side].at[pl.ds(start, count)]
            out.append(
                pltpu.make_async_remote_copy(
                    source, target, hop_sems.at[leg, at], hop_sems.at[leg, at],
                    device_id={"lane": jnp.int32(lane_to)}, device_id_type=MESH,
                )
            )
        return out

    def all_hops(leg, stage, entry):
        per_route = [hops_of(leg, stage, entry, route) for route in range(len(entry[3]))]
        return [copy for copies in per_route for copy in copies]

    def straight(stage, k, arriving=False):
        at = stage * len(SIDES) + k
        over = at if arriving else at + 1 - 2 * k
        part = pl.ds(0, split(stage)[0])
        return pltpu.make_async_remote_copy(
            send_bufs[at].at[part], recv_bufs[over].at[part],
            send_sem.at[sem_of(stage, k)], recv_sem.at[sem_of(stage, over % len(SIDES))],
            device_id=targets[k], device_id_type=MESH,
        )

    slow = [lane == entry[0] for entry in SLOW]
    slow_side = {entry[1]: i for i, entry in enumerate(SLOW)}
    whole = [
        there & jnp.logical_not(slow[slow_side[k]]) if k in slow_side else there
        for k, there in enumerate(exists)
    ]

    hurried = slow[0] | slow[1]

    def crosses(k):
        for i, entry in enumerate(SLOW):
            if SIDES[k][1] == entry[2] - entry[0]:
                return slow[i]
        return None

    def in_one(stage, k):
        if k in slow_side:
            return whole[k]
        if stage in CORNERS_BY_SIDES and k >= 4:
            return exists[k] & crosses(k)
        return exists[k]

    def in_parts(stage, k):
        if k not in slow_side or any(corners for _, _, _, corners in STAGES[stage]):
            return None
        return slow[slow_side[k]]

    def send_across(stage, refs):
        for k in STAGE_SIDES[stage]:
            if crosses(k) is None:
                continue

            @pl.when(exists[k] & crosses(k))
            def _():
                pack(send_bufs[stage * len(SIDES) + k], refs, STAGES[stage], SIDES[k])
                if k in slow_side:
                    for copy in all_hops(0, stage, SLOW[slow_side[k]]):
                        copy.start()
                    straight(stage, k).start()
                else:
                    copy_of(stage, k).start()

    relays = jnp.bool_(False)
    for entry in SLOW:
        for between in entry[3]:
            relays = relays | (lane == between)

    def send(stage, refs, sides=None, among=None):
        for k in STAGE_SIDES[stage] if sides is None else sides:
            there = exists[k] if among is None else exists[k] & among
            if crosses(k) is not None:
                there = there & jnp.logical_not(crosses(k))

            @pl.when(there)
            def _():
                pack(send_bufs[stage * len(SIDES) + k], refs, STAGES[stage], SIDES[k])
                copy_of(stage, k).start()

    def pass_on(stage):
        for entry in SLOW:
            for route, between in enumerate(entry[3]):
                if CHUNKS[stage][route]:

                    @pl.when(lane == between)
                    def _():
                        for first, second in zip(
                            hops_of(0, stage, entry, route), hops_of(1, stage, entry, route)
                        ):
                            first.wait_recv()
                            second.start()

    def receive(stage, refs, sides=(2, 3, 4, 5, 6, 7, 0, 1)):
        for k in sides:
            if k not in STAGE_SIDES[stage]:
                continue

            @pl.when(in_one(stage, k))
            def _():
                copy_of(stage, k, arriving=True).wait_recv()
                if in_parts(stage, k) is None:
                    unpack(recv_bufs[stage * len(SIDES) + k], refs, STAGES[stage], SIDES[k])

            if in_parts(stage, k) is not None:

                @pl.when(in_parts(stage, k))
                def _():
                    straight(stage, k, arriving=True).wait_recv()
                    for copy in all_hops(1, stage, SLOW[1 - slow_side[k]]):
                        copy.wait_recv()

                @pl.when(exists[k])
                def _():
                    unpack(recv_bufs[stage * len(SIDES) + k], refs, STAGES[stage], SIDES[k])

    total = jnp.int32(0)
    for there in exists:
        total = total + there.astype(jnp.int32)
    for far, _, _, betweens in SLOW:
        total = total + (lane == far).astype(jnp.int32) * len(betweens)
    with jax.named_scope("barrier"):
        pl.semaphore_wait(barrier, total)

    with jax.named_scope("cross_am"):
        send_across(0, (u0, gain, base))
        send_across(1, (coarse_gain,))
    with jax.named_scope("send_a"):
        send(0, (u0, gain, base))

    wide = ((-DU, 9),)

    def restrict(low, high, groups):
        def restrict_row(y, carry):
            for x in groups:

                def u_at(dy, dx):
                    return u3[pl.ds(FINE.at(2 * y + dy, 2 * x + dx), 8, stride=2), :]

                def own(ref, dy, dx):
                    return ref[pl.ds((2 * y + dy) * N + 2 * x + dx, 8, stride=2), :]

                block = {}
                for dy in range(2):
                    for dx in range(2):
                        block[dy, dx] = u_at(dy, dx)
                total = None
                for dy in range(2):
                    for dx in range(2):
                        here = block[dy, dx]
                        around = (
                            u_at(dy, -1 if dx == 0 else 2) + u_at(-1 if dy == 0 else 2, dx)
                        ) + (block[dy, 1 - dx] + block[1 - dy, dx])
                        defect = (own(source, dy, dx) + around) - (4.0 + own(mass, dy, dx)) * here
                        total = defect if total is None else total + defect
                at = pl.multiple_of(COARSE.at(y, x), 8)
                coarse_base[pl.ds(at, 8), :] = coarse_gain[pl.ds(at, 8), :] * (0.5 * total)
            return carry

        lax.fori_loop(low, high, restrict_row, 0)

    with jax.named_scope("inside"):
        sweep(FINE, u0, u1, gain, base, wide, 1, N - 1)
        sweep(FINE, u1, u2, gain, base, wide, 2, N - 2)
        sweep(FINE, u2, u3, gain, base, wide, 3, N - 3)
        restrict(RIM, M - RIM, range(0, M, 8))
    with jax.named_scope("cross_e"):
        send_across(2, (coarse_base,))
        send(1, (coarse_gain,), ALL[:4], hurried)
    with jax.named_scope("pass_a"):
        pass_on(0)
    with jax.named_scope("pass_m"):
        pass_on(1)
    with jax.named_scope("send_m_early"):
        send(1, (coarse_gain,), ALL[:4], relays)
    with jax.named_scope("receive_a"):
        receive(0, (u0, gain, base))
    with jax.named_scope("pass_e"):
        pass_on(2)
    with jax.named_scope("send_me"):
        send(1, (coarse_gain,), ALL[:4], jnp.logical_not(relays | hurried))
        send(2, (coarse_base,), ALL[:4], jnp.logical_not(hurried))
    with jax.named_scope("rim"):
        for step, (src, dst) in enumerate(((u0, u1), (u1, u2), (u2, u3))):
            for at in (step - 3, N - 1 - step):
                sweep(FINE, src, dst, gain, base, wide, at, at + 4)
                sweep_strip(FINE, src, dst, gain, base, at, 4)
        restrict(0, RIM, range(0, M, 8))
        restrict(M - RIM, M, range(0, M, 8))
        restrict(RIM, M - RIM, (0, M - 8))
    with jax.named_scope("send_l"):
        send_across(3, (coarse_base,))
        send(2, (coarse_base,), ALL[:4], hurried)
        send(3, (coarse_base,))
        send_across(4, (u3,))
        send(4, (u3,))
    with jax.named_scope("receive_my"):
        receive(1, (coarse_gain,), (2, 3))
        send(5, (coarse_gain,))
    with jax.named_scope("receive_ey"):
        receive(2, (coarse_base,), (2, 3))
        send(6, (coarse_base,))
    with jax.named_scope("receive_m"):
        receive(1, (coarse_gain,), (4, 5, 6, 7, 0, 1))
        receive(5, (coarse_gain,))
    with jax.named_scope("receive_e"):
        receive(2, (coarse_base,), (4, 5, 6, 7, 0, 1))
        receive(6, (coarse_base,))
    with jax.named_scope("receive_l"):
        receive(3, (coarse_base,))

    with jax.named_scope("coarse"):
        src, dst = coarse_base, c0
        for step in range(1, INNER):
            depth = DC - step
            span = M + 2 * depth
            if span > 56:
                groups = ((-depth, 4), (-depth + 32, 4))
            else:
                groups = ((-depth, -(-span // 8)),)
            sweep(COARSE, src, dst, coarse_gain, coarse_base, groups, -depth, M + depth)
            src, dst = dst, (c1 if dst is c0 else c0)
    coarse = src

    for k in range(4):

        @pl.when(jnp.logical_not(exists[k]))
        def _():
            clear(u3, FINE, SIDES[k], DV)

    with jax.named_scope("receive_v"):
        receive(4, (u3,))

    def prolong_row(i, carry):
        y = i - 2
        for x in (-2, 6, 14, 22, M - 6):
            add = coarse[pl.ds(COARSE.at(y, x), 8), :]
            for dy in range(2):
                for dx in range(2):
                    at = pl.ds(FINE.at(2 * y + dy, 2 * x + dx), 8, stride=2)
                    u0[at, :] = u3[at, :] + add
        return carry

    with jax.named_scope("prolong"):
        lax.fori_loop(0, M + 4, prolong_row, 0)
    with jax.named_scope("after"):
        sweep(FINE, u0, u1, gain, base, wide, -2, N + 2)
        sweep(FINE, u1, u0, gain, base, wide, -1, N + 1)
        stores = []
        for i in range(PARTS):
            low, high = i * N // PARTS, (i + 1) * N // PARTS
            sweep(
                FINE, u0, result, gain, base, ((0, 4), (32, 4)), low, high,
                store_at=lambda y, x: y * N + x,
            )
            part = pl.ds(low * N, (high - low) * N)
            stores.append(pltpu.make_async_copy(result.at[part], out_ref.at[part], store_sem.at[i]))
            stores[-1].start()

    for store in stores:
        store.wait()
    for stage in range(len(STAGES)):
        for k in STAGE_SIDES[stage]:

            if in_parts(stage, k) is not None:

                @pl.when(in_parts(stage, k))
                def _():
                    for copy in all_hops(0, stage, SLOW[slow_side[k]]):
                        copy.wait_send()
                    straight(stage, k).wait_send()

            @pl.when(in_one(stage, k))
            def _():
                copy_of(stage, k).wait_send()

        for entry in SLOW:
            for route, between in enumerate(entry[3]):
                if CHUNKS[stage][route]:

                    @pl.when(lane == between)
                    def _():
                        for copy in hops_of(1, stage, entry, route):
                            copy.wait_send()


def per_device(source_terms, initial_values, absorption):
    shape = source_terms.shape
    flat = [
        pltpu.with_memory_space_constraint(x.reshape(N * N, CASES), pltpu.HBM)
        for x in (source_terms, initial_values, absorption)
    ]
    vmem = lambda count: pltpu.VMEM((count, CASES), jnp.float32)
    buffers = [
        vmem(message_rows(parts, side) if k in sides else 8)
        for parts, sides in zip(STAGES, STAGE_SIDES)
        for k, side in enumerate(SIDES)
    ]
    result = pl.pallas_call(
        kernel,
        out_shape=pltpu.VMEM((N * N, CASES), jnp.float32),
        in_specs=[pl.BlockSpec(memory_space=pltpu.HBM)] * 3,
        out_specs=pl.BlockSpec(memory_space=pl.ANY),
        scratch_shapes=[vmem(N * N)] * 3
        + [vmem(SIZE_F)] * 6
        + [vmem(SIZE_C)] * 4
        + buffers
        + buffers
        + [vmem(max(8, *(sum(route) for route in routes))) for routes in CHUNKS]
        + [
            pltpu.SemaphoreType.DMA((3,)),
            pltpu.SemaphoreType.DMA((len(SEMS),)),
            pltpu.SemaphoreType.DMA((len(SEMS),)),
            pltpu.SemaphoreType.DMA((2, len(HOPS))),
            pltpu.SemaphoreType.DMA((PARTS,)),
            vmem(N * N),
        ],
        compiler_params=pltpu.CompilerParams(
            collective_id=0, has_side_effects=True, vmem_limit_bytes=48 << 20
        ),
        name="cycle",
    )(*flat)
    return result.reshape(shape)


def solution(mesh):
    placed = P(("shift", "band"), "lane", None)
    return jax.shard_map(
        per_device,
        mesh=mesh,
        in_specs=(placed,) * 3,
        out_specs=placed,
        check_vma=False,
    )
```

```python
import jax
import jax.numpy as jnp
from jax import lax
from jax.experimental import pallas as pl
from jax.experimental.pallas import tpu as pltpu
from jax.sharding import PartitionSpec as P

CASES = 128
BEFORE = 3
AFTER = 3
INNER = 13
N = 64
M = N // 2
DU = BEFORE + 1
DW = BEFORE
DV = AFTER
DC = INNER + 1
DM = INNER

PF, YF, XF = 88, 4, 8
SIZE_F = (N + 2 * YF) * PF
PC, YC, XC = 72, 14, 16
SIZE_C = (M + 2 * YC) * PC

SLOW = ((7, 1, 8, (4, 6, 5)), (8, 0, 7, (11, 9, 10)))
CHUNKS = (
    ((104, 104,), (72, 72,), (88, 88,)),
    ((144,), (136,), (136,)),
    ((112,), (112,), (112,)),
    ((), (), ()),
    ((), (), ()),
    ((), (), ()),
    ((), (), ()),
)
SIDES = ((0, -1), (0, 1), (-1, 0), (1, 0), (-1, -1), (-1, 1), (1, -1), (1, 1))
MESH = pl.DeviceIdType.MESH


def sem_of(stage, k):
    return SEMS.index(sem_key(stage, k))


def sem_key(stage, k):
    if stage in CORNERS_BY_SIDES and k >= 4:
        return stage, "corner", SIDES[k][0]
    return stage, "side", k


def split(stage):
    first = message_rows(STAGES[stage], (0, 1)) - sum(sum(route) for route in CHUNKS[stage])
    at, routes = first, []
    for route in CHUNKS[stage]:
        routes.append([])
        for count in route:
            routes[-1].append((at, count))
            at += count
    return first, routes


HOPS = [
    (stage, route, chunk)
    for stage in range(len(CHUNKS))
    for route in range(len(CHUNKS[stage]))
    for chunk in range(len(CHUNKS[stage][route]))
]


class Grid:
    def __init__(self, size, pitch, y_off, x_off):
        self.size, self.pitch, self.y_off, self.x_off = size, pitch, y_off, x_off

    def at(self, y, x):
        return (y + self.y_off) * self.pitch + x + self.x_off


FINE = Grid(N, PF, YF, XF)
COARSE = Grid(M, PC, YC, XC)


def runs(grid, side, boxes, sending):
    def place(sign, low, high, own):
        n = grid.size
        if sign == 0:
            return low, high - low
        if own:
            return (n - high if sign > 0 else low - 1), high - low + 1
        return (n - 1 + low if sign > 0 else -high), high - low + 1

    out = []
    for y_range, x_range, along_x in boxes:
        y, height = place(side[0], *y_range, sending[0])
        x, width = place(side[1], *x_range, sending[1])
        if along_x:
            out += [(grid.at(y + i, x), width, 1) for i in range(height)]
        else:
            out += [(grid.at(y, x + i), height, grid.pitch) for i in range(width)]
    return out


def whole_halo(grid, side, depth):
    own = (0, grid.size)
    if side[0] == 0:
        return [(own, (1, depth), False)]
    if side[1] == 0:
        return [((1, depth), own, True)]
    return [((1, depth - dx), (dx, dx), False) for dx in range(1, depth)]


PARTS = 4
RIM = 2


def early_halo(grid, side, depth):
    own, deep = (RIM, grid.size - RIM), (RIM + 1, depth)
    if side[0] == 0:
        return [(own, deep, False)]
    if side[1] == 0:
        return [(deep, own, True)]
    return [((RIM + 1, depth - dx), (dx, dx), False) for dx in range(RIM + 1, depth - RIM)]


def late_halo(grid, side, depth):
    n = grid.size
    own, near, deep = (0, n), (1, RIM), (RIM + 1, depth)
    ends = [(0, RIM), (n - RIM, n)]
    if side[0] == 0:
        return [(own, near, False)] + [(end, deep, True) for end in ends]
    if side[1] == 0:
        return [(near, own, True)] + [(deep, end, False) for end in ends]
    return [((1, depth - dx), (dx, dx), False) for dx in range(1, RIM + 1)] + [
        ((dy, dy), (RIM + 1, depth - dy), True) for dy in range(1, RIM + 1)
    ]


def far_halo(grid, side, depth):
    own = (0, grid.size)
    if side[0] == 0:
        return [(own, (2, depth), False)]
    if side[1] == 0:
        return [((2, depth), own, True)]
    return whole_halo(grid, side, depth)


def pieces(part, side, sending):
    grid, depth, boxes, corners = part
    if not corners:
        return runs(grid, side, boxes(grid, side, depth), (sending, sending))
    both = [(sy, side[1]) for sy in (-1, 1)]
    return [
        run
        for corner in both
        for run in runs(grid, corner, boxes(grid, corner, depth), (False, sending))
    ]


def message_rows(parts, side):
    total = sum(
        count for part in parts for _, count, _ in pieces(part, side, True)
    )
    return -(-total // 8) * 8


def rows(start, count, stride):
    return pl.ds(start, count) if stride == 1 else pl.ds(start, count, stride=stride)


def pack(buffer, refs, parts, side):
    at = 0
    for ref, part in zip(refs, parts):
        for start, count, stride in pieces(part, side, True):
            buffer[pl.ds(at, count), :] = ref[rows(start, count, stride), :]
            at += count


def unpack(buffer, refs, parts, side):
    at = 0
    for ref, part in zip(refs, parts):
        for start, count, stride in pieces(part, side, False):
            ref[rows(start, count, stride), :] = buffer[pl.ds(at, count), :]
            at += count


def clear(ref, grid, side, depth):
    sy, sx = side
    n = grid.size
    if sy == 0:
        for i in range(depth):
            x = n + i if sx > 0 else -1 - i
            count = n + 2 * grid.y_off
            ref[pl.ds(grid.at(-grid.y_off, x), count, stride=grid.pitch), :] = jnp.zeros(
                (count, CASES), jnp.float32
            )
    else:
        y0 = n if sy > 0 else -depth
        count = depth * grid.pitch
        ref[pl.ds(grid.at(y0, -grid.x_off), count), :] = jnp.zeros((count, CASES), jnp.float32)


STAGES = (
    tuple((FINE, depth, whole_halo, False) for depth in (DU, DW, DW)),
    ((COARSE, DM, whole_halo, False),),
    ((COARSE, DC, early_halo, False),),
    ((COARSE, DC, late_halo, False),),
    ((FINE, DV, far_halo, False),),
    ((COARSE, DM, whole_halo, True),),
    ((COARSE, DC, early_halo, True),),
)
ALL = (1, 0, 2, 3, 4, 5, 6, 7)
CORNERS_FIRST = (1, 0, 4, 5, 6, 7, 2, 3)
STAGE_SIDES = (CORNERS_FIRST, ALL, ALL, CORNERS_FIRST, CORNERS_FIRST, ALL[:2], ALL[:2])
CORNERS_BY_SIDES = (1, 2)
SEMS = list(dict.fromkeys(sem_key(stage, k) for stage, ks in enumerate(STAGE_SIDES) for k in ks))


def sweep(grid, src, dst, gain, base, groups, y_low, y_high, store_at=None):
    store_at = store_at or grid.at
    count = y_high - y_low
    unroll = min(range(min(count, 7), min(count, 10) + 1), key=lambda n: (-(-count // n) * n, -n))
    blocks = -(-count // unroll)

    def block(i, carry):
        y = jnp.minimum(y_low + i * unroll, y_high - unroll)
        row = grid.at(y, 0)
        out_row = store_at(y, 0)
        out_pitch = store_at(1, 0) - store_at(0, 0)
        for x0, width in groups:

            def load(ref, dy, x):
                return ref[pl.ds(row + dy * grid.pitch + x0 + x, 8, stride=width), :]

            left = [load(src, k, -1) for k in range(unroll)]
            here = [load(src, k, 0) for k in range(unroll)]
            for x in range(width):
                right = [load(src, k, x + 1) for k in range(unroll)]
                above = load(src, -1, x)
                below = load(src, unroll, x)
                for k in range(unroll):
                    up = here[k - 1] if k else above
                    down = here[k + 1] if k + 1 < unroll else below
                    around = (left[k] + right[k]) + (up + down)
                    new = (
                        0.2 * here[k] + load(base, k, x) + load(gain, k, x) * around
                    )
                    dst[pl.ds(out_row + k * out_pitch + x0 + x, 8, stride=width), :] = new
                left, here = here, right
        return carry

    lax.fori_loop(0, blocks, block, 0)


def sweep_strip(grid, src, dst, gain, base, x0, width):
    def block(i, carry):
        row = grid.at(8 * i, x0)

        def load(ref, dy, x):
            return ref[pl.ds(row + dy * grid.pitch + x, 8, stride=grid.pitch), :]

        left, here = load(src, 0, -1), load(src, 0, 0)
        for x in range(width):
            right = load(src, 0, x + 1)
            around = (left + right) + (load(src, -1, x) + load(src, 1, x))
            new = 0.2 * here + load(base, 0, x) + load(gain, 0, x) * around
            dst[pl.ds(row + x, 8, stride=grid.pitch), :] = new
            left, here = here, right
        return carry

    lax.fori_loop(0, grid.size // 8, block, 0)


def kernel(source_hbm, values_hbm, mass_hbm, out_ref, source, start, mass, u0, u1, u2, u3, gain, base,
           coarse_gain, c0, c1, coarse_base, *rest):
    counts = len(STAGES) * len(SIDES)
    send_bufs, recv_bufs = rest[:counts], rest[counts : 2 * counts]
    held = rest[2 * counts : 2 * counts + len(STAGES)]
    load_sem, send_sem, recv_sem, hop_sems, store_sem, result = rest[2 * counts + len(STAGES) :]
    band, lane = lax.axis_index("band"), lax.axis_index("lane")
    bands, lanes = lax.axis_size("band"), lax.axis_size("lane")

    loads = [
        pltpu.make_async_copy(src, dst, load_sem.at[i])
        for i, (src, dst) in enumerate(
            ((mass_hbm, mass), (source_hbm, source), (values_hbm, start))
        )
    ]
    for copy in loads:
        copy.start()

    exists, targets = [], []
    for sy, sx in SIDES:
        y, x = band + sy, lane + sx
        exists.append((y >= 0) & (y < bands) & (x >= 0) & (x < lanes))
        targets.append({"band": y, "lane": x})

    barrier = pltpu.get_barrier_semaphore()
    for there, target in zip(exists, targets):

        @pl.when(there)
        def _():
            pl.semaphore_signal(barrier, inc=1, device_id=target, device_id_type=MESH)

    def tell(lane_to):
        pl.semaphore_signal(
            barrier, inc=1, device_id={"lane": jnp.int32(lane_to)}, device_id_type=MESH
        )

    for far, _, _, betweens in SLOW:
        for between in betweens:

            @pl.when(lane == between)
            def _():
                tell(far)

    for k in range(4):

        @pl.when(jnp.logical_not(exists[k]))
        def _():
            for ref, grid, depth in (
                (u0, FINE, DU), (gain, FINE, DW), (base, FINE, DW),
                (coarse_gain, COARSE, DM), (coarse_base, COARSE, DC),
            ):
                clear(ref, grid, SIDES[k], depth)

    loads[0].wait()

    def coarse_row(y, carry):
        for x in range(0, M, 8):
            total = None
            for dy in range(2):
                for dx in range(2):
                    part = mass[pl.ds((2 * y + dy) * N + 2 * x + dx, 8, stride=2), :]
                    total = part if total is None else total + part
            at = pl.multiple_of(COARSE.at(y, x), 8)
            coarse_gain[pl.ds(at, 8), :] = 0.8 / (4.0 + 0.5 * total)
        return carry

    with jax.named_scope("coarse_setup"):
        lax.fori_loop(0, M, coarse_row, 0)
    with jax.named_scope("load"):
        loads[1].wait()
        loads[2].wait()

    def fine_row(y, carry):
        for x in range(0, N, 8):
            here = pl.ds(pl.multiple_of(y * N + x, 8), 8)
            there = pl.ds(pl.multiple_of(FINE.at(y, x), 8), 8)
            factor = 0.8 / (4.0 + mass[here, :])
            gain[there, :] = factor
            base[there, :] = factor * source[here, :]
            u0[there, :] = start[here, :]
        return carry

    with jax.named_scope("fine_setup"):
        lax.fori_loop(0, N, fine_row, 0)

    def copy_of(stage, k, arriving=False):
        at = stage * len(SIDES) + k
        sy, sx = SIDES[k]
        over = at if arriving else stage * len(SIDES) + SIDES.index((-sy, -sx))
        return pltpu.make_async_remote_copy(
            send_bufs[at], recv_bufs[over],
            send_sem.at[sem_of(stage, k)], recv_sem.at[sem_of(stage, over % len(SIDES))],
            device_id=targets[k], device_id_type=MESH,
        )

    def hops_of(leg, stage, entry, route):
        _, side, other, betweens = entry
        chunks = split(stage)[1][route]
        out = []
        for i, (start, count) in enumerate(chunks):
            at = HOPS.index((stage, route, i))
            here = held[stage].at[pl.ds(start - chunks[0][0], count)]
            if leg == 0:
                source = send_bufs[stage * len(SIDES) + side].at[pl.ds(start, count)]
                target, lane_to = here, betweens[route]
            else:
                source, lane_to = here, other
                target = recv_bufs[stage * len(SIDES) + 1 - side].at[pl.ds(start, count)]
            out.append(
                pltpu.make_async_remote_copy(
                    source, target, hop_sems.at[leg, at], hop_sems.at[leg, at],
                    device_id={"lane": jnp.int32(lane_to)}, device_id_type=MESH,
                )
            )
        return out

    def all_hops(leg, stage, entry):
        per_route = [hops_of(leg, stage, entry, route) for route in range(len(entry[3]))]
        return [copy for copies in per_route for copy in copies]

    def straight(stage, k, arriving=False):
        at = stage * len(SIDES) + k
        over = at if arriving else at + 1 - 2 * k
        part = pl.ds(0, split(stage)[0])
        return pltpu.make_async_remote_copy(
            send_bufs[at].at[part], recv_bufs[over].at[part],
            send_sem.at[sem_of(stage, k)], recv_sem.at[sem_of(stage, over % len(SIDES))],
            device_id=targets[k], device_id_type=MESH,
        )

    slow = [lane == entry[0] for entry in SLOW]
    slow_side = {entry[1]: i for i, entry in enumerate(SLOW)}
    whole = [
        there & jnp.logical_not(slow[slow_side[k]]) if k in slow_side else there
        for k, there in enumerate(exists)
    ]

    hurried = slow[0] | slow[1]

    def crosses(k):
        for i, entry in enumerate(SLOW):
            if SIDES[k][1] == entry[2] - entry[0]:
                return slow[i]
        return None

    def in_one(stage, k):
        if k in slow_side:
            return whole[k]
        if stage in CORNERS_BY_SIDES and k >= 4:
            return exists[k] & crosses(k)
        return exists[k]

    def in_parts(stage, k):
        if k not in slow_side or any(corners for _, _, _, corners in STAGES[stage]):
            return None
        return slow[slow_side[k]]

    def send_across(stage, refs):
        for k in STAGE_SIDES[stage]:
            if crosses(k) is None:
                continue

            @pl.when(exists[k] & crosses(k))
            def _():
                pack(send_bufs[stage * len(SIDES) + k], refs, STAGES[stage], SIDES[k])
                if k in slow_side:
                    for copy in all_hops(0, stage, SLOW[slow_side[k]]):
                        copy.start()
                    if split(stage)[0]:
                        straight(stage, k).start()
                else:
                    copy_of(stage, k).start()

    relays = jnp.bool_(False)
    for entry in SLOW:
        for between in entry[3]:
            relays = relays | (lane == between)

    def send(stage, refs, sides=None, among=None):
        for k in STAGE_SIDES[stage] if sides is None else sides:
            there = exists[k] if among is None else exists[k] & among
            if crosses(k) is not None:
                there = there & jnp.logical_not(crosses(k))

            @pl.when(there)
            def _():
                pack(send_bufs[stage * len(SIDES) + k], refs, STAGES[stage], SIDES[k])
                copy_of(stage, k).start()

    def pass_on(stage):
        for entry in SLOW:
            for route, between in enumerate(entry[3]):
                if CHUNKS[stage][route]:

                    @pl.when(lane == between)
                    def _():
                        for first, second in zip(
                            hops_of(0, stage, entry, route), hops_of(1, stage, entry, route)
                        ):
                            first.wait_recv()
                            second.start()

    def receive(stage, refs, sides=(2, 3, 4, 5, 6, 7, 0, 1)):
        for k in sides:
            if k not in STAGE_SIDES[stage]:
                continue

            @pl.when(in_one(stage, k))
            def _():
                copy_of(stage, k, arriving=True).wait_recv()
                if in_parts(stage, k) is None:
                    unpack(recv_bufs[stage * len(SIDES) + k], refs, STAGES[stage], SIDES[k])

            if in_parts(stage, k) is not None:

                @pl.when(in_parts(stage, k))
                def _():
                    if split(stage)[0]:
                        straight(stage, k, arriving=True).wait_recv()
                    for copy in all_hops(1, stage, SLOW[1 - slow_side[k]]):
                        copy.wait_recv()

                @pl.when(exists[k])
                def _():
                    unpack(recv_bufs[stage * len(SIDES) + k], refs, STAGES[stage], SIDES[k])

    total = jnp.int32(0)
    for there in exists:
        total = total + there.astype(jnp.int32)
    for far, _, _, betweens in SLOW:
        total = total + (lane == far).astype(jnp.int32) * len(betweens)
    with jax.named_scope("barrier"):
        pl.semaphore_wait(barrier, total)

    with jax.named_scope("cross_am"):
        send_across(0, (u0, gain, base))
        send_across(1, (coarse_gain,))
    with jax.named_scope("send_a"):
        send(0, (u0, gain, base))

    wide = ((-DU, 9),)

    def restrict(low, high, groups):
        def restrict_row(y, carry):
            for x in groups:

                def u_at(dy, dx):
                    return u3[pl.ds(FINE.at(2 * y + dy, 2 * x + dx), 8, stride=2), :]

                def own(ref, dy, dx):
                    return ref[pl.ds((2 * y + dy) * N + 2 * x + dx, 8, stride=2), :]

                block = {}
                for dy in range(2):
                    for dx in range(2):
                        block[dy, dx] = u_at(dy, dx)
                total = None
                for dy in range(2):
                    for dx in range(2):
                        here = block[dy, dx]
                        around = (
                            u_at(dy, -1 if dx == 0 else 2) + u_at(-1 if dy == 0 else 2, dx)
                        ) + (block[dy, 1 - dx] + block[1 - dy, dx])
                        defect = (own(source, dy, dx) + around) - (4.0 + own(mass, dy, dx)) * here
                        total = defect if total is None else total + defect
                at = pl.multiple_of(COARSE.at(y, x), 8)
                coarse_base[pl.ds(at, 8), :] = coarse_gain[pl.ds(at, 8), :] * (0.5 * total)
            return carry

        lax.fori_loop(low, high, restrict_row, 0)

    with jax.named_scope("inside"):
        sweep(FINE, u0, u1, gain, base, wide, 1, N - 1)
        sweep(FINE, u1, u2, gain, base, wide, 2, N - 2)
        sweep(FINE, u2, u3, gain, base, wide, 3, N - 3)
        restrict(RIM, M - RIM, range(0, M, 8))
    with jax.named_scope("cross_e"):
        send_across(2, (coarse_base,))
        send(1, (coarse_gain,), ALL[:4], hurried)
    with jax.named_scope("pass_a"):
        pass_on(0)
    with jax.named_scope("pass_m"):
        pass_on(1)
    with jax.named_scope("send_m_early"):
        send(1, (coarse_gain,), ALL[:4], relays)
    with jax.named_scope("receive_a"):
        receive(0, (u0, gain, base))
    with jax.named_scope("pass_e"):
        pass_on(2)
    with jax.named_scope("send_me"):
        send(1, (coarse_gain,), ALL[:4], jnp.logical_not(relays | hurried))
        send(2, (coarse_base,), ALL[:4], jnp.logical_not(hurried))
    with jax.named_scope("rim"):
        for step, (src, dst) in enumerate(((u0, u1), (u1, u2), (u2, u3))):
            for at in (step - 3, N - 1 - step):
                sweep(FINE, src, dst, gain, base, wide, at, at + 4)
                sweep_strip(FINE, src, dst, gain, base, at, 4)
        restrict(0, RIM, range(0, M, 8))
        restrict(M - RIM, M, range(0, M, 8))
        restrict(RIM, M - RIM, (0, M - 8))
    with jax.named_scope("send_l"):
        send_across(3, (coarse_base,))
        send(2, (coarse_base,), ALL[:4], hurried)
        send(3, (coarse_base,))
        send_across(4, (u3,))
        send(4, (u3,))
    with jax.named_scope("receive_my"):
        receive(1, (coarse_gain,), (2, 3))
        send(5, (coarse_gain,))
    with jax.named_scope("receive_ey"):
        receive(2, (coarse_base,), (2, 3))
        send(6, (coarse_base,))
    with jax.named_scope("receive_m"):
        receive(1, (coarse_gain,), (4, 5, 6, 7, 0, 1))
        receive(5, (coarse_gain,))
    with jax.named_scope("receive_e"):
        receive(2, (coarse_base,), (4, 5, 6, 7, 0, 1))
        receive(6, (coarse_base,))
    with jax.named_scope("receive_l"):
        receive(3, (coarse_base,))

    with jax.named_scope("coarse"):
        src, dst = coarse_base, c0
        for step in range(1, INNER):
            depth = DC - step
            span = M + 2 * depth
            if span > 56:
                groups = ((-depth, 4), (-depth + 32, 4))
            else:
                groups = ((-depth, -(-span // 8)),)
            sweep(COARSE, src, dst, coarse_gain, coarse_base, groups, -depth, M + depth)
            src, dst = dst, (c1 if dst is c0 else c0)
    coarse = src

    for k in range(4):

        @pl.when(jnp.logical_not(exists[k]))
        def _():
            clear(u3, FINE, SIDES[k], DV)

    with jax.named_scope("receive_v"):
        receive(4, (u3,))

    def prolong_row(i, carry):
        y = i - 2
        for x in (-2, 6, 14, 22, M - 6):
            add = coarse[pl.ds(COARSE.at(y, x), 8), :]
            for dy in range(2):
                for dx in range(2):
                    at = pl.ds(FINE.at(2 * y + dy, 2 * x + dx), 8, stride=2)
                    u0[at, :] = u3[at, :] + add
        return carry

    with jax.named_scope("prolong"):
        lax.fori_loop(0, M + 4, prolong_row, 0)
    with jax.named_scope("after"):
        sweep(FINE, u0, u1, gain, base, wide, -2, N + 2)
        sweep(FINE, u1, u0, gain, base, wide, -1, N + 1)
        stores = []
        for i in range(PARTS):
            low, high = i * N // PARTS, (i + 1) * N // PARTS
            sweep(
                FINE, u0, result, gain, base, ((0, 4), (32, 4)), low, high,
                store_at=lambda y, x: y * N + x,
            )
            part = pl.ds(low * N, (high - low) * N)
            stores.append(pltpu.make_async_copy(result.at[part], out_ref.at[part], store_sem.at[i]))
            stores[-1].start()

    for store in stores:
        store.wait()
    for stage in range(len(STAGES)):
        for k in STAGE_SIDES[stage]:

            if in_parts(stage, k) is not None:

                @pl.when(in_parts(stage, k))
                def _():
                    for copy in all_hops(0, stage, SLOW[slow_side[k]]):
                        copy.wait_send()
                    if split(stage)[0]:
                        straight(stage, k).wait_send()

            @pl.when(in_one(stage, k))
            def _():
                copy_of(stage, k).wait_send()

        for entry in SLOW:
            for route, between in enumerate(entry[3]):
                if CHUNKS[stage][route]:

                    @pl.when(lane == between)
                    def _():
                        for copy in hops_of(1, stage, entry, route):
                            copy.wait_send()


def per_device(source_terms, initial_values, absorption):
    shape = source_terms.shape
    flat = [
        pltpu.with_memory_space_constraint(x.reshape(N * N, CASES), pltpu.HBM)
        for x in (source_terms, initial_values, absorption)
    ]
    vmem = lambda count: pltpu.VMEM((count, CASES), jnp.float32)
    buffers = [
        vmem(message_rows(parts, side) if k in sides else 8)
        for parts, sides in zip(STAGES, STAGE_SIDES)
        for k, side in enumerate(SIDES)
    ]
    result = pl.pallas_call(
        kernel,
        out_shape=pltpu.VMEM((N * N, CASES), jnp.float32),
        in_specs=[pl.BlockSpec(memory_space=pltpu.HBM)] * 3,
        out_specs=pl.BlockSpec(memory_space=pl.ANY),
        scratch_shapes=[vmem(N * N)] * 3
        + [vmem(SIZE_F)] * 6
        + [vmem(SIZE_C)] * 4
        + buffers
        + buffers
        + [vmem(max(8, *(sum(route) for route in routes))) for routes in CHUNKS]
        + [
            pltpu.SemaphoreType.DMA((3,)),
            pltpu.SemaphoreType.DMA((len(SEMS),)),
            pltpu.SemaphoreType.DMA((len(SEMS),)),
            pltpu.SemaphoreType.DMA((2, len(HOPS))),
            pltpu.SemaphoreType.DMA((PARTS,)),
            vmem(N * N),
        ],
        compiler_params=pltpu.CompilerParams(
            collective_id=0, has_side_effects=True, vmem_limit_bytes=48 << 20
        ),
        name="cycle",
    )(*flat)
    return result.reshape(shape)


def solution(mesh):
    placed = P(("shift", "band"), "lane", None)
    return jax.shard_map(
        per_device,
        mesh=mesh,
        in_specs=(placed,) * 3,
        out_specs=placed,
        check_vma=False,
    )
```

```python
import jax
import jax.numpy as jnp
from jax import lax
from jax.experimental import pallas as pl
from jax.experimental.pallas import tpu as pltpu
from jax.sharding import PartitionSpec as P

CASES = 128
BEFORE = 3
AFTER = 3
INNER = 13
N = 64
M = N // 2
DU = BEFORE + 1
DW = BEFORE
DV = AFTER
DC = INNER + 1
DM = INNER

PF, YF, XF = 88, 4, 8
SIZE_F = (N + 2 * YF) * PF
PC, YC, XC = 72, 14, 16
SIZE_C = (M + 2 * YC) * PC

SLOW = ((7, 1, 8, (4, 6, 5)), (8, 0, 7, (11, 9, 10)))
CHUNKS = (
    ((104, 104,), (72, 72,), (80, 80,)),
    ((152,), (128,), (136,)),
    ((120,), (96,), (120,)),
    ((), (), ()),
    ((), (), ()),
    ((), (), ()),
    ((), (), ()),
)
SIDES = ((0, -1), (0, 1), (-1, 0), (1, 0), (-1, -1), (-1, 1), (1, -1), (1, 1))
MESH = pl.DeviceIdType.MESH


def sem_of(stage, k):
    return SEMS.index(sem_key(stage, k))


def sem_key(stage, k):
    if stage in CORNERS_BY_SIDES and k >= 4:
        return stage, "corner", SIDES[k][0]
    return stage, "side", k


def split(stage):
    first = message_rows(STAGES[stage], (0, 1)) - sum(sum(route) for route in CHUNKS[stage])
    at, routes = first, []
    for route in CHUNKS[stage]:
        routes.append([])
        for count in route:
            routes[-1].append((at, count))
            at += count
    return first, routes


HOPS = [
    (stage, route, chunk)
    for stage in range(len(CHUNKS))
    for route in range(len(CHUNKS[stage]))
    for chunk in range(len(CHUNKS[stage][route]))
]


class Grid:
    def __init__(self, size, pitch, y_off, x_off):
        self.size, self.pitch, self.y_off, self.x_off = size, pitch, y_off, x_off

    def at(self, y, x):
        return (y + self.y_off) * self.pitch + x + self.x_off


FINE = Grid(N, PF, YF, XF)
COARSE = Grid(M, PC, YC, XC)


def runs(grid, side, boxes, sending):
    def place(sign, low, high, own):
        n = grid.size
        if sign == 0:
            return low, high - low
        if own:
            return (n - high if sign > 0 else low - 1), high - low + 1
        return (n - 1 + low if sign > 0 else -high), high - low + 1

    out = []
    for y_range, x_range, along_x in boxes:
        y, height = place(side[0], *y_range, sending[0])
        x, width = place(side[1], *x_range, sending[1])
        if along_x:
            out += [(grid.at(y + i, x), width, 1) for i in range(height)]
        else:
            out += [(grid.at(y, x + i), height, grid.pitch) for i in range(width)]
    return out


def whole_halo(grid, side, depth):
    own = (0, grid.size)
    if side[0] == 0:
        return [(own, (1, depth), False)]
    if side[1] == 0:
        return [((1, depth), own, True)]
    return [((1, depth - dx), (dx, dx), False) for dx in range(1, depth)]


PARTS = 4
RIM = 2


def early_halo(grid, side, depth):
    own, deep = (RIM, grid.size - RIM), (RIM + 1, depth)
    if side[0] == 0:
        return [(own, deep, False)]
    if side[1] == 0:
        return [(deep, own, True)]
    return [((RIM + 1, depth - dx), (dx, dx), False) for dx in range(RIM + 1, depth - RIM)]


def late_halo(grid, side, depth):
    n = grid.size
    own, near, deep = (0, n), (1, RIM), (RIM + 1, depth)
    ends = [(0, RIM), (n - RIM, n)]
    if side[0] == 0:
        return [(own, near, False)] + [(end, deep, True) for end in ends]
    if side[1] == 0:
        return [(near, own, True)] + [(deep, end, False) for end in ends]
    return [((1, depth - dx), (dx, dx), False) for dx in range(1, RIM + 1)] + [
        ((dy, dy), (RIM + 1, depth - dy), True) for dy in range(1, RIM + 1)
    ]


def far_halo(grid, side, depth):
    own = (0, grid.size)
    if side[0] == 0:
        return [(own, (2, depth), False)]
    if side[1] == 0:
        return [((2, depth), own, True)]
    return whole_halo(grid, side, depth)


def pieces(part, side, sending):
    grid, depth, boxes, corners = part
    if not corners:
        return runs(grid, side, boxes(grid, side, depth), (sending, sending))
    both = [(sy, side[1]) for sy in (-1, 1)]
    return [
        run
        for corner in both
        for run in runs(grid, corner, boxes(grid, corner, depth), (False, sending))
    ]


def message_rows(parts, side):
    total = sum(
        count for part in parts for _, count, _ in pieces(part, side, True)
    )
    return -(-total // 8) * 8


def rows(start, count, stride):
    return pl.ds(start, count) if stride == 1 else pl.ds(start, count, stride=stride)


def pack(buffer, refs, parts, side):
    at = 0
    for ref, part in zip(refs, parts):
        for start, count, stride in pieces(part, side, True):
            buffer[pl.ds(at, count), :] = ref[rows(start, count, stride), :]
            at += count


def unpack(buffer, refs, parts, side):
    at = 0
    for ref, part in zip(refs, parts):
        for start, count, stride in pieces(part, side, False):
            ref[rows(start, count, stride), :] = buffer[pl.ds(at, count), :]
            at += count


def clear(ref, grid, side, depth):
    sy, sx = side
    n = grid.size
    if sy == 0:
        for i in range(depth):
            x = n + i if sx > 0 else -1 - i
            count = n + 2 * grid.y_off
            ref[pl.ds(grid.at(-grid.y_off, x), count, stride=grid.pitch), :] = jnp.zeros(
                (count, CASES), jnp.float32
            )
    else:
        y0 = n if sy > 0 else -depth
        count = depth * grid.pitch
        ref[pl.ds(grid.at(y0, -grid.x_off), count), :] = jnp.zeros((count, CASES), jnp.float32)


STAGES = (
    tuple((FINE, depth, whole_halo, False) for depth in (DU, DW, DW)),
    ((COARSE, DM, whole_halo, False),),
    ((COARSE, DC, early_halo, False),),
    ((COARSE, DC, late_halo, False),),
    ((FINE, DV, far_halo, False),),
    ((COARSE, DM, whole_halo, True),),
    ((COARSE, DC, early_halo, True),),
)
ALL = (1, 0, 2, 3, 4, 5, 6, 7)
CORNERS_FIRST = (1, 0, 4, 5, 6, 7, 2, 3)
STAGE_SIDES = (CORNERS_FIRST, ALL, ALL, CORNERS_FIRST, CORNERS_FIRST, ALL[:2], ALL[:2])
CORNERS_BY_SIDES = (1, 2)
SEMS = list(dict.fromkeys(sem_key(stage, k) for stage, ks in enumerate(STAGE_SIDES) for k in ks))


def sweep(grid, src, dst, gain, base, groups, y_low, y_high, store_at=None):
    store_at = store_at or grid.at
    count = y_high - y_low
    unroll = min(range(min(count, 7), min(count, 10) + 1), key=lambda n: (-(-count // n) * n, -n))
    blocks = -(-count // unroll)

    def block(i, carry):
        y = jnp.minimum(y_low + i * unroll, y_high - unroll)
        row = grid.at(y, 0)
        out_row = store_at(y, 0)
        out_pitch = store_at(1, 0) - store_at(0, 0)
        for x0, width in groups:

            def load(ref, dy, x):
                return ref[pl.ds(row + dy * grid.pitch + x0 + x, 8, stride=width), :]

            left = [load(src, k, -1) for k in range(unroll)]
            here = [load(src, k, 0) for k in range(unroll)]
            for x in range(width):
                right = [load(src, k, x + 1) for k in range(unroll)]
                above = load(src, -1, x)
                below = load(src, unroll, x)
                for k in range(unroll):
                    up = here[k - 1] if k else above
                    down = here[k + 1] if k + 1 < unroll else below
                    around = (left[k] + right[k]) + (up + down)
                    new = (
                        0.2 * here[k] + load(base, k, x) + load(gain, k, x) * around
                    )
                    dst[pl.ds(out_row + k * out_pitch + x0 + x, 8, stride=width), :] = new
                left, here = here, right
        return carry

    lax.fori_loop(0, blocks, block, 0)


def sweep_strips(grid, src, dst, gain, base, starts, width, blocks=2):
    def step(i, carry):
        for j in range(blocks):
            for x0 in starts:
                row = grid.at(8 * (i * blocks + j), x0)

                def load(ref, dy, x):
                    return ref[pl.ds(row + dy * grid.pitch + x, 8, stride=grid.pitch), :]

                left, here = load(src, 0, -1), load(src, 0, 0)
                for x in range(width):
                    right = load(src, 0, x + 1)
                    around = (left + right) + (load(src, -1, x) + load(src, 1, x))
                    new = 0.2 * here + load(base, 0, x) + load(gain, 0, x) * around
                    dst[pl.ds(row + x, 8, stride=grid.pitch), :] = new
                    left, here = here, right
        return carry

    lax.fori_loop(0, grid.size // 8 // blocks, step, 0)


def kernel(source_hbm, values_hbm, mass_hbm, out_ref, source, start, mass, u0, u1, u2, u3, gain, base,
           coarse_gain, c0, c1, coarse_base, *rest):
    counts = len(STAGES) * len(SIDES)
    send_bufs, recv_bufs = rest[:counts], rest[counts : 2 * counts]
    held = rest[2 * counts : 2 * counts + len(STAGES)]
    load_sem, send_sem, recv_sem, hop_sems, store_sem, result = rest[2 * counts + len(STAGES) :]
    band, lane = lax.axis_index("band"), lax.axis_index("lane")
    bands, lanes = lax.axis_size("band"), lax.axis_size("lane")

    loads = [
        pltpu.make_async_copy(src, dst, load_sem.at[i])
        for i, (src, dst) in enumerate(
            ((mass_hbm, mass), (source_hbm, source), (values_hbm, start))
        )
    ]
    for copy in loads:
        copy.start()

    exists, targets = [], []
    for sy, sx in SIDES:
        y, x = band + sy, lane + sx
        exists.append((y >= 0) & (y < bands) & (x >= 0) & (x < lanes))
        targets.append({"band": y, "lane": x})

    barrier = pltpu.get_barrier_semaphore()
    for there, target in zip(exists, targets):

        @pl.when(there)
        def _():
            pl.semaphore_signal(barrier, inc=1, device_id=target, device_id_type=MESH)

    def tell(lane_to):
        pl.semaphore_signal(
            barrier, inc=1, device_id={"lane": jnp.int32(lane_to)}, device_id_type=MESH
        )

    for far, _, _, betweens in SLOW:
        for between in betweens:

            @pl.when(lane == between)
            def _():
                tell(far)

    for k in range(4):

        @pl.when(jnp.logical_not(exists[k]))
        def _():
            for ref, grid, depth in (
                (u0, FINE, DU), (gain, FINE, DW), (base, FINE, DW),
                (coarse_gain, COARSE, DM), (coarse_base, COARSE, DC),
            ):
                clear(ref, grid, SIDES[k], depth)

    loads[0].wait()

    def coarse_row(y, carry):
        for x in range(0, M, 8):
            total = None
            for dy in range(2):
                for dx in range(2):
                    part = mass[pl.ds((2 * y + dy) * N + 2 * x + dx, 8, stride=2), :]
                    total = part if total is None else total + part
            at = pl.multiple_of(COARSE.at(y, x), 8)
            coarse_gain[pl.ds(at, 8), :] = 0.8 / (4.0 + 0.5 * total)
        return carry

    with jax.named_scope("coarse_setup"):
        lax.fori_loop(0, M, coarse_row, 0)
    with jax.named_scope("load"):
        loads[1].wait()
        loads[2].wait()

    def fine_cells(steps, cells):
        def fine_step(i, carry):
            for y, x in cells(i):
                here = pl.ds(pl.multiple_of(y * N + x, 8), 8)
                there = pl.ds(pl.multiple_of(FINE.at(y, x), 8), 8)
                factor = 0.8 / (4.0 + mass[here, :])
                gain[there, :] = factor
                base[there, :] = factor * source[here, :]
                u0[there, :] = start[here, :]
            return carry

        lax.fori_loop(0, steps, fine_step, 0)

    with jax.named_scope("fine_setup"):
        fine_cells(DU, lambda i: [(y, x) for y in (i, N - DU + i) for x in range(0, N, 8)])
        fine_cells(
            (N - 2 * DU) // 8,
            lambda i: [(DU + 8 * i + j, x) for j in range(8) for x in (0, N - 8)],
        )

    def copy_of(stage, k, arriving=False):
        at = stage * len(SIDES) + k
        sy, sx = SIDES[k]
        over = at if arriving else stage * len(SIDES) + SIDES.index((-sy, -sx))
        return pltpu.make_async_remote_copy(
            send_bufs[at], recv_bufs[over],
            send_sem.at[sem_of(stage, k)], recv_sem.at[sem_of(stage, over % len(SIDES))],
            device_id=targets[k], device_id_type=MESH,
        )

    def hops_of(leg, stage, entry, route):
        _, side, other, betweens = entry
        chunks = split(stage)[1][route]
        out = []
        for i, (start, count) in enumerate(chunks):
            at = HOPS.index((stage, route, i))
            here = held[stage].at[pl.ds(start - chunks[0][0], count)]
            if leg == 0:
                source = send_bufs[stage * len(SIDES) + side].at[pl.ds(start, count)]
                target, lane_to = here, betweens[route]
            else:
                source, lane_to = here, other
                target = recv_bufs[stage * len(SIDES) + 1 - side].at[pl.ds(start, count)]
            out.append(
                pltpu.make_async_remote_copy(
                    source, target, hop_sems.at[leg, at], hop_sems.at[leg, at],
                    device_id={"lane": jnp.int32(lane_to)}, device_id_type=MESH,
                )
            )
        return out

    def all_hops(leg, stage, entry):
        per_route = [hops_of(leg, stage, entry, route) for route in range(len(entry[3]))]
        return [copy for copies in per_route for copy in copies]

    def straight(stage, k, arriving=False):
        at = stage * len(SIDES) + k
        over = at if arriving else at + 1 - 2 * k
        part = pl.ds(0, split(stage)[0])
        return pltpu.make_async_remote_copy(
            send_bufs[at].at[part], recv_bufs[over].at[part],
            send_sem.at[sem_of(stage, k)], recv_sem.at[sem_of(stage, over % len(SIDES))],
            device_id=targets[k], device_id_type=MESH,
        )

    slow = [lane == entry[0] for entry in SLOW]
    slow_side = {entry[1]: i for i, entry in enumerate(SLOW)}
    whole = [
        there & jnp.logical_not(slow[slow_side[k]]) if k in slow_side else there
        for k, there in enumerate(exists)
    ]

    hurried = slow[0] | slow[1]

    def crosses(k):
        for i, entry in enumerate(SLOW):
            if SIDES[k][1] == entry[2] - entry[0]:
                return slow[i]
        return None

    def in_one(stage, k):
        if k in slow_side:
            return whole[k]
        if stage in CORNERS_BY_SIDES and k >= 4:
            return exists[k] & crosses(k)
        return exists[k]

    def in_parts(stage, k):
        if k not in slow_side or any(corners for _, _, _, corners in STAGES[stage]):
            return None
        return slow[slow_side[k]]

    def send_across(stage, refs):
        for k in STAGE_SIDES[stage]:
            if crosses(k) is None:
                continue

            @pl.when(exists[k] & crosses(k))
            def _():
                pack(send_bufs[stage * len(SIDES) + k], refs, STAGES[stage], SIDES[k])
                if k in slow_side:
                    for copy in all_hops(0, stage, SLOW[slow_side[k]]):
                        copy.start()
                    if split(stage)[0]:
                        straight(stage, k).start()
                else:
                    copy_of(stage, k).start()

    relays = jnp.bool_(False)
    for entry in SLOW:
        for between in entry[3]:
            relays = relays | (lane == between)

    def send(stage, refs, sides=None, among=None):
        for k in STAGE_SIDES[stage] if sides is None else sides:
            there = exists[k] if among is None else exists[k] & among
            if crosses(k) is not None:
                there = there & jnp.logical_not(crosses(k))

            @pl.when(there)
            def _():
                pack(send_bufs[stage * len(SIDES) + k], refs, STAGES[stage], SIDES[k])
                copy_of(stage, k).start()

    def pass_on(stage):
        for entry in SLOW:
            for route, between in enumerate(entry[3]):
                if CHUNKS[stage][route]:

                    @pl.when(lane == between)
                    def _():
                        for first, second in zip(
                            hops_of(0, stage, entry, route), hops_of(1, stage, entry, route)
                        ):
                            first.wait_recv()
                            second.start()

    def receive(stage, refs, sides=(2, 3, 4, 5, 6, 7, 0, 1)):
        for k in sides:
            if k not in STAGE_SIDES[stage]:
                continue

            @pl.when(in_one(stage, k))
            def _():
                copy_of(stage, k, arriving=True).wait_recv()
                if in_parts(stage, k) is None:
                    unpack(recv_bufs[stage * len(SIDES) + k], refs, STAGES[stage], SIDES[k])

            if in_parts(stage, k) is not None:

                @pl.when(in_parts(stage, k))
                def _():
                    if split(stage)[0]:
                        straight(stage, k, arriving=True).wait_recv()
                    for copy in all_hops(1, stage, SLOW[1 - slow_side[k]]):
                        copy.wait_recv()

                @pl.when(exists[k])
                def _():
                    unpack(recv_bufs[stage * len(SIDES) + k], refs, STAGES[stage], SIDES[k])

    total = jnp.int32(0)
    for there in exists:
        total = total + there.astype(jnp.int32)
    for far, _, _, betweens in SLOW:
        total = total + (lane == far).astype(jnp.int32) * len(betweens)
    with jax.named_scope("barrier"):
        pl.semaphore_wait(barrier, total)

    with jax.named_scope("cross_am"):
        send_across(0, (u0, gain, base))
        send_across(1, (coarse_gain,))
    with jax.named_scope("send_a"):
        send(0, (u0, gain, base))

    wide = ((-DU, 9),)

    def restrict(low, high, groups, each=1):
        def restrict_rows(i, carry):
            for y, x in [(low + i * each + j, x) for j in range(each) for x in groups]:

                def u_at(dy, dx):
                    return u3[pl.ds(FINE.at(2 * y + dy, 2 * x + dx), 8, stride=2), :]

                def own(ref, dy, dx):
                    return ref[pl.ds((2 * y + dy) * N + 2 * x + dx, 8, stride=2), :]

                block = {}
                for dy in range(2):
                    for dx in range(2):
                        block[dy, dx] = u_at(dy, dx)
                total = None
                for dy in range(2):
                    for dx in range(2):
                        here = block[dy, dx]
                        around = (
                            u_at(dy, -1 if dx == 0 else 2) + u_at(-1 if dy == 0 else 2, dx)
                        ) + (block[dy, 1 - dx] + block[1 - dy, dx])
                        defect = (own(source, dy, dx) + around) - (4.0 + own(mass, dy, dx)) * here
                        total = defect if total is None else total + defect
                at = pl.multiple_of(COARSE.at(y, x), 8)
                coarse_base[pl.ds(at, 8), :] = coarse_gain[pl.ds(at, 8), :] * (0.5 * total)
            return carry

        lax.fori_loop(0, (high - low) // each, restrict_rows, 0)

    with jax.named_scope("inside"):
        fine_cells(
            (N - 2 * DU) // 2,
            lambda i: [(DU + 2 * i + j, x) for j in range(2) for x in range(8, N - 8, 8)],
        )
        sweep(FINE, u0, u1, gain, base, wide, 1, N - 1)
        sweep(FINE, u1, u2, gain, base, wide, 2, N - 2)
        sweep(FINE, u2, u3, gain, base, wide, 3, N - 3)
        restrict(RIM, M - RIM, range(0, M, 8))
    with jax.named_scope("cross_e"):
        send_across(2, (coarse_base,))
        send(1, (coarse_gain,), ALL[:4], hurried)
        send(2, (coarse_base,), ALL[:4], hurried)
    with jax.named_scope("pass_a"):
        pass_on(0)
    with jax.named_scope("pass_m"):
        pass_on(1)
    with jax.named_scope("send_m_early"):
        send(1, (coarse_gain,), ALL[:4], relays)
        send(2, (coarse_base,), ALL[:4], relays)
    with jax.named_scope("receive_a"):
        receive(0, (u0, gain, base))
    with jax.named_scope("pass_e"):
        pass_on(2)
    with jax.named_scope("send_me"):
        send(1, (coarse_gain,), ALL[:4], jnp.logical_not(relays | hurried))
        send(2, (coarse_base,), ALL[:4], jnp.logical_not(relays | hurried))
    with jax.named_scope("rim"):
        for step, (src, dst) in enumerate(((u0, u1), (u1, u2), (u2, u3))):
            ends = (step - 3, N - 1 - step)
            for at in ends:
                sweep(FINE, src, dst, gain, base, wide, at, at + 4)
            sweep_strips(FINE, src, dst, gain, base, ends, 4)
        restrict(0, RIM, range(0, M, 8))
        restrict(M - RIM, M, range(0, M, 8))
        restrict(RIM, M - RIM, (0, M - 8), 2)
    with jax.named_scope("send_l"):
        send_across(3, (coarse_base,))
        send(3, (coarse_base,))
        send_across(4, (u3,))
        send(4, (u3,))
    with jax.named_scope("receive_my"):
        receive(1, (coarse_gain,), (2, 3))
        send(5, (coarse_gain,))
    with jax.named_scope("receive_ey"):
        receive(2, (coarse_base,), (2, 3))
        send(6, (coarse_base,))
    with jax.named_scope("receive_m"):
        receive(1, (coarse_gain,), (4, 5, 6, 7, 0, 1))
        receive(5, (coarse_gain,))
    with jax.named_scope("receive_e"):
        receive(2, (coarse_base,), (4, 5, 6, 7, 0, 1))
        receive(6, (coarse_base,))
    with jax.named_scope("receive_l"):
        receive(3, (coarse_base,))

    with jax.named_scope("coarse"):
        src, dst = coarse_base, c0
        for step in range(1, INNER):
            depth = DC - step
            span = M + 2 * depth
            if span > 56:
                groups = ((-depth, 4), (-depth + 32, 4))
            else:
                groups = ((-depth, -(-span // 8)),)
            sweep(COARSE, src, dst, coarse_gain, coarse_base, groups, -depth, M + depth)
            src, dst = dst, (c1 if dst is c0 else c0)
    coarse = src

    for k in range(4):

        @pl.when(jnp.logical_not(exists[k]))
        def _():
            clear(u3, FINE, SIDES[k], DV)

    with jax.named_scope("receive_v"):
        receive(4, (u3,))

    def prolong_row(i, carry):
        y = i - 2
        for x in (-2, 6, 14, 22, M - 6):
            add = coarse[pl.ds(COARSE.at(y, x), 8), :]
            for dy in range(2):
                for dx in range(2):
                    at = pl.ds(FINE.at(2 * y + dy, 2 * x + dx), 8, stride=2)
                    u0[at, :] = u3[at, :] + add
        return carry

    with jax.named_scope("prolong"):
        lax.fori_loop(0, M + 4, prolong_row, 0)
    with jax.named_scope("after"):
        sweep(FINE, u0, u1, gain, base, wide, -2, N + 2)
        sweep(FINE, u1, u0, gain, base, wide, -1, N + 1)
        stores = []
        for i in range(PARTS):
            low, high = i * N // PARTS, (i + 1) * N // PARTS
            sweep(
                FINE, u0, result, gain, base, ((0, 4), (32, 4)), low, high,
                store_at=lambda y, x: y * N + x,
            )
            part = pl.ds(low * N, (high - low) * N)
            stores.append(pltpu.make_async_copy(result.at[part], out_ref.at[part], store_sem.at[i]))
            stores[-1].start()

    for store in stores:
        store.wait()
    for stage in range(len(STAGES)):
        for k in STAGE_SIDES[stage]:

            if in_parts(stage, k) is not None:

                @pl.when(in_parts(stage, k))
                def _():
                    for copy in all_hops(0, stage, SLOW[slow_side[k]]):
                        copy.wait_send()
                    if split(stage)[0]:
                        straight(stage, k).wait_send()

            @pl.when(in_one(stage, k))
            def _():
                copy_of(stage, k).wait_send()

        for entry in SLOW:
            for route, between in enumerate(entry[3]):
                if CHUNKS[stage][route]:

                    @pl.when(lane == between)
                    def _():
                        for copy in hops_of(1, stage, entry, route):
                            copy.wait_send()


def per_device(source_terms, initial_values, absorption):
    shape = source_terms.shape
    flat = [
        pltpu.with_memory_space_constraint(x.reshape(N * N, CASES), pltpu.HBM)
        for x in (source_terms, initial_values, absorption)
    ]
    vmem = lambda count: pltpu.VMEM((count, CASES), jnp.float32)
    buffers = [
        vmem(message_rows(parts, side) if k in sides else 8)
        for parts, sides in zip(STAGES, STAGE_SIDES)
        for k, side in enumerate(SIDES)
    ]
    result = pl.pallas_call(
        kernel,
        out_shape=pltpu.VMEM((N * N, CASES), jnp.float32),
        in_specs=[pl.BlockSpec(memory_space=pltpu.HBM)] * 3,
        out_specs=pl.BlockSpec(memory_space=pl.ANY),
        scratch_shapes=[vmem(N * N)] * 3
        + [vmem(SIZE_F)] * 6
        + [vmem(SIZE_C)] * 4
        + buffers
        + buffers
        + [vmem(max(8, *(sum(route) for route in routes))) for routes in CHUNKS]
        + [
            pltpu.SemaphoreType.DMA((3,)),
            pltpu.SemaphoreType.DMA((len(SEMS),)),
            pltpu.SemaphoreType.DMA((len(SEMS),)),
            pltpu.SemaphoreType.DMA((2, len(HOPS))),
            pltpu.SemaphoreType.DMA((PARTS,)),
            vmem(N * N),
        ],
        compiler_params=pltpu.CompilerParams(
            collective_id=0, has_side_effects=True, vmem_limit_bytes=48 << 20
        ),
        name="cycle",
    )(*flat)
    return result.reshape(shape)


def solution(mesh):
    placed = P(("shift", "band"), "lane", None)
    return jax.shard_map(
        per_device,
        mesh=mesh,
        in_specs=(placed,) * 3,
        out_specs=placed,
        check_vma=False,
    )
```

```python
import jax
import jax.numpy as jnp
from jax import lax
from jax.experimental import pallas as pl
from jax.experimental.pallas import tpu as pltpu
from jax.sharding import PartitionSpec as P

CASES = 128
BEFORE = 3
AFTER = 3
INNER = 13
N = 64
M = N // 2
DU = BEFORE + 1
DW = BEFORE
DV = AFTER
DC = INNER + 1
DM = INNER

PF, YF, XF = 88, 4, 8
SIZE_F = (N + 2 * YF + 8) * PF
PC, YC, XC = 72, 14, 16
SIZE_C = (M + 2 * YC + 8) * PC

SLOW = ((7, 1, 8, (4, 6, 5)), (8, 0, 7, (11, 9, 10)))
CHUNKS = (
    ((104, 104,), (72, 72,), (80, 80,)),
    ((152,), (128,), (136,)),
    ((120,), (96,), (120,)),
    ((), (), ()),
    ((), (), ()),
    ((), (), ()),
    ((), (), ()),
)
SIDES = ((0, -1), (0, 1), (-1, 0), (1, 0), (-1, -1), (-1, 1), (1, -1), (1, 1))
MESH = pl.DeviceIdType.MESH


def sem_of(stage, k):
    return SEMS.index(sem_key(stage, k))


def sem_key(stage, k):
    if stage in CORNERS_BY_SIDES and k >= 4:
        return stage, "corner", SIDES[k][0]
    return stage, "side", k


def split(stage):
    first = message_rows(STAGES[stage], (0, 1)) - sum(sum(route) for route in CHUNKS[stage])
    at, routes = first, []
    for route in CHUNKS[stage]:
        routes.append([])
        for count in route:
            routes[-1].append((at, count))
            at += count
    return first, routes


HOPS = [
    (stage, route, chunk)
    for stage in range(len(CHUNKS))
    for route in range(len(CHUNKS[stage]))
    for chunk in range(len(CHUNKS[stage][route]))
]


class Grid:
    def __init__(self, size, pitch, y_off, x_off):
        self.size, self.pitch, self.y_off, self.x_off = size, pitch, y_off, x_off

    def at(self, y, x):
        return (y + self.y_off) * self.pitch + x + self.x_off


FINE = Grid(N, PF, YF, XF)
COARSE = Grid(M, PC, YC, XC)


def runs(grid, side, boxes, sending):
    def place(sign, low, high, own):
        n = grid.size
        if sign == 0:
            return low, high - low
        if own:
            return (n - high if sign > 0 else low - 1), high - low + 1
        return (n - 1 + low if sign > 0 else -high), high - low + 1

    out = []
    for y_range, x_range, along_x in boxes:
        y, height = place(side[0], *y_range, sending[0])
        x, width = place(side[1], *x_range, sending[1])
        if along_x:
            out += [(grid.at(y + i, x), width, 1) for i in range(height)]
        else:
            out += [(grid.at(y, x + i), height, grid.pitch) for i in range(width)]
    return out


def whole_halo(grid, side, depth):
    own = (0, grid.size)
    if side[0] == 0:
        return [(own, (1, depth), False)]
    if side[1] == 0:
        return [((1, depth), own, True)]
    return [((1, depth - dx), (dx, dx), False) for dx in range(1, depth)]


PARTS = 4
RIM = 2


def early_halo(grid, side, depth):
    own, deep = (RIM, grid.size - RIM), (RIM + 1, depth)
    if side[0] == 0:
        return [(own, deep, False)]
    if side[1] == 0:
        return [(deep, own, True)]
    return [((RIM + 1, depth - dx), (dx, dx), False) for dx in range(RIM + 1, depth - RIM)]


def late_halo(grid, side, depth):
    n = grid.size
    own, near, deep = (0, n), (1, RIM), (RIM + 1, depth)
    ends = [(0, RIM), (n - RIM, n)]
    if side[0] == 0:
        return [(own, near, False)] + [(end, deep, True) for end in ends]
    if side[1] == 0:
        return [(near, own, True)] + [(deep, end, False) for end in ends]
    return [((1, depth - dx), (dx, dx), False) for dx in range(1, RIM + 1)] + [
        ((dy, dy), (RIM + 1, depth - dy), True) for dy in range(1, RIM + 1)
    ]


def far_halo(grid, side, depth):
    own = (0, grid.size)
    if side[0] == 0:
        return [(own, (2, depth), False)]
    if side[1] == 0:
        return [((2, depth), own, True)]
    return whole_halo(grid, side, depth)


def pieces(part, side, sending):
    grid, depth, boxes, corners = part
    if not corners:
        return runs(grid, side, boxes(grid, side, depth), (sending, sending))
    both = [(sy, side[1]) for sy in (-1, 1)]
    return [
        run
        for corner in both
        for run in runs(grid, corner, boxes(grid, corner, depth), (False, sending))
    ]


def message_rows(parts, side):
    total = sum(
        count for part in parts for _, count, _ in pieces(part, side, True)
    )
    return -(-total // 8) * 8


def rows(start, count, stride):
    return pl.ds(start, count) if stride == 1 else pl.ds(start, count, stride=stride)


def pack(buffer, refs, parts, side):
    at = 0
    for ref, part in zip(refs, parts):
        for start, count, stride in pieces(part, side, True):
            buffer[pl.ds(at, count), :] = ref[rows(start, count, stride), :]
            at += count


def unpack(buffer, refs, parts, side):
    at = 0
    for ref, part in zip(refs, parts):
        for start, count, stride in pieces(part, side, False):
            ref[rows(start, count, stride), :] = buffer[pl.ds(at, count), :]
            at += count


def clear(ref, grid, side, depth):
    sy, sx = side
    n = grid.size
    if sy == 0:
        for i in range(depth):
            x = n + i if sx > 0 else -1 - i
            count = n + 2 * grid.y_off
            ref[pl.ds(grid.at(-grid.y_off, x), count, stride=grid.pitch), :] = jnp.zeros(
                (count, CASES), jnp.float32
            )
    else:
        y0 = n if sy > 0 else -depth
        count = depth * grid.pitch
        ref[pl.ds(grid.at(y0, -grid.x_off), count), :] = jnp.zeros((count, CASES), jnp.float32)


STAGES = (
    tuple((FINE, depth, whole_halo, False) for depth in (DU, DW, DW)),
    ((COARSE, DM, whole_halo, False),),
    ((COARSE, DC, early_halo, False),),
    ((COARSE, DC, late_halo, False),),
    ((FINE, DV, far_halo, False),),
    ((COARSE, DM, whole_halo, True),),
    ((COARSE, DC, early_halo, True),),
)
ALL = (1, 0, 2, 3, 4, 5, 6, 7)
CORNERS_FIRST = (1, 0, 4, 5, 6, 7, 2, 3)
STAGE_SIDES = (CORNERS_FIRST, ALL, ALL, CORNERS_FIRST, CORNERS_FIRST, ALL[:2], ALL[:2])
CORNERS_BY_SIDES = (1, 2)
SEMS = list(dict.fromkeys(sem_key(stage, k) for stage, ks in enumerate(STAGE_SIDES) for k in ks))


def sweep(grid, src, dst, gain, base, groups, y_low, y_high, store_at=None):
    store_at = store_at or grid.at
    count = y_high - y_low
    unroll = min(range(min(count, 7), min(count, 10) + 1), key=lambda n: (-(-count // n) * n, -n))
    blocks = -(-count // unroll)

    def block(i, carry):
        y = jnp.minimum(y_low + i * unroll, y_high - unroll)
        row = grid.at(y, 0)
        out_row = store_at(y, 0)
        out_pitch = store_at(1, 0) - store_at(0, 0)
        for x0, width in groups:

            def load(ref, dy, x):
                return ref[pl.ds(row + dy * grid.pitch + x0 + x, 8, stride=width), :]

            left = [load(src, k, -1) for k in range(unroll)]
            here = [load(src, k, 0) for k in range(unroll)]
            for x in range(width):
                right = [load(src, k, x + 1) for k in range(unroll)]
                above = load(src, -1, x)
                below = load(src, unroll, x)
                for k in range(unroll):
                    up = here[k - 1] if k else above
                    down = here[k + 1] if k + 1 < unroll else below
                    around = (left[k] + right[k]) + (up + down)
                    new = (
                        0.2 * here[k] + load(base, k, x) + load(gain, k, x) * around
                    )
                    dst[pl.ds(out_row + k * out_pitch + x0 + x, 8, stride=width), :] = new
                left, here = here, right
        return carry

    lax.fori_loop(0, blocks, block, 0)


def sweep_strips(grid, src, dst, gain, base, starts, width, blocks=2):
    def step(i, carry):
        for j in range(blocks):
            for x0 in starts:
                row = grid.at(8 * (i * blocks + j), x0)

                def load(ref, dy, x):
                    return ref[pl.ds(row + dy * grid.pitch + x, 8, stride=grid.pitch), :]

                left, here = load(src, 0, -1), load(src, 0, 0)
                for x in range(width):
                    right = load(src, 0, x + 1)
                    around = (left + right) + (load(src, -1, x) + load(src, 1, x))
                    new = 0.2 * here + load(base, 0, x) + load(gain, 0, x) * around
                    dst[pl.ds(row + x, 8, stride=grid.pitch), :] = new
                    left, here = here, right
        return carry

    lax.fori_loop(0, grid.size // 8 // blocks, step, 0)


def kernel(source_hbm, values_hbm, mass_hbm, out_ref, source, start, mass, u0, u1, u2, u3, gain, base,
           coarse_gain, c0, c1, coarse_base, *rest):
    counts = len(STAGES) * len(SIDES)
    send_bufs, recv_bufs = rest[:counts], rest[counts : 2 * counts]
    held = rest[2 * counts : 2 * counts + len(STAGES)]
    load_sem, send_sem, recv_sem, hop_sems, store_sem, result = rest[2 * counts + len(STAGES) :]
    band, lane = lax.axis_index("band"), lax.axis_index("lane")
    bands, lanes = lax.axis_size("band"), lax.axis_size("lane")

    loads = [
        pltpu.make_async_copy(src, dst.at[pl.ds(0, N * N)], load_sem.at[i])
        for i, (src, dst) in enumerate(
            ((mass_hbm, mass), (source_hbm, source), (values_hbm, start))
        )
    ]
    for copy in loads:
        copy.start()

    exists, targets = [], []
    for sy, sx in SIDES:
        y, x = band + sy, lane + sx
        exists.append((y >= 0) & (y < bands) & (x >= 0) & (x < lanes))
        targets.append({"band": y, "lane": x})

    barrier = pltpu.get_barrier_semaphore()
    for there, target in zip(exists, targets):

        @pl.when(there)
        def _():
            pl.semaphore_signal(barrier, inc=1, device_id=target, device_id_type=MESH)

    def tell(lane_to):
        pl.semaphore_signal(
            barrier, inc=1, device_id={"lane": jnp.int32(lane_to)}, device_id_type=MESH
        )

    for far, _, _, betweens in SLOW:
        for between in betweens:

            @pl.when(lane == between)
            def _():
                tell(far)

    for k in range(4):

        @pl.when(jnp.logical_not(exists[k]))
        def _():
            for ref, grid, depth in (
                (u0, FINE, DU), (gain, FINE, DW), (base, FINE, DW),
                (coarse_gain, COARSE, DM), (coarse_base, COARSE, DC),
            ):
                clear(ref, grid, SIDES[k], depth)

    loads[0].wait()

    def coarse_row(y, carry):
        for x in range(0, M, 8):
            total = None
            for dy in range(2):
                for dx in range(2):
                    part = mass[pl.ds((2 * y + dy) * N + 2 * x + dx, 8, stride=2), :]
                    total = part if total is None else total + part
            at = pl.multiple_of(COARSE.at(y, x), 8)
            coarse_gain[pl.ds(at, 8), :] = 0.8 / (4.0 + 0.5 * total)
        return carry

    with jax.named_scope("coarse_setup"):
        lax.fori_loop(0, M, coarse_row, 0)
    with jax.named_scope("load"):
        loads[1].wait()
        loads[2].wait()

    def fine_cells(steps, cells):
        def fine_step(i, carry):
            for y, x in cells(i):
                here = pl.ds(pl.multiple_of(y * N + x, 8), 8)
                there = pl.ds(pl.multiple_of(FINE.at(y, x), 8), 8)
                factor = 0.8 / (4.0 + mass[here, :])
                gain[there, :] = factor
                base[there, :] = factor * source[here, :]
                u0[there, :] = start[here, :]
            return carry

        lax.fori_loop(0, steps, fine_step, 0)

    with jax.named_scope("fine_setup"):
        fine_cells(DU, lambda i: [(y, x) for y in (i, N - DU + i) for x in range(0, N, 8)])
        fine_cells(
            (N - 2 * DU) // 8,
            lambda i: [(DU + 8 * i + j, x) for j in range(8) for x in (0, N - 8)],
        )

    def copy_of(stage, k, arriving=False):
        at = stage * len(SIDES) + k
        sy, sx = SIDES[k]
        over = at if arriving else stage * len(SIDES) + SIDES.index((-sy, -sx))
        part = pl.ds(0, message_rows(STAGES[stage], SIDES[k]))
        return pltpu.make_async_remote_copy(
            send_bufs[at].at[part], recv_bufs[over].at[part],
            send_sem.at[sem_of(stage, k)], recv_sem.at[sem_of(stage, over % len(SIDES))],
            device_id=targets[k], device_id_type=MESH,
        )

    def hops_of(leg, stage, entry, route):
        _, side, other, betweens = entry
        chunks = split(stage)[1][route]
        out = []
        for i, (start, count) in enumerate(chunks):
            at = HOPS.index((stage, route, i))
            here = held[stage].at[pl.ds(start - chunks[0][0], count)]
            if leg == 0:
                source = send_bufs[stage * len(SIDES) + side].at[pl.ds(start, count)]
                target, lane_to = here, betweens[route]
            else:
                source, lane_to = here, other
                target = recv_bufs[stage * len(SIDES) + 1 - side].at[pl.ds(start, count)]
            out.append(
                pltpu.make_async_remote_copy(
                    source, target, hop_sems.at[leg, at], hop_sems.at[leg, at],
                    device_id={"lane": jnp.int32(lane_to)}, device_id_type=MESH,
                )
            )
        return out

    def all_hops(leg, stage, entry):
        per_route = [hops_of(leg, stage, entry, route) for route in range(len(entry[3]))]
        return [copy for copies in per_route for copy in copies]

    def straight(stage, k, arriving=False):
        at = stage * len(SIDES) + k
        over = at if arriving else at + 1 - 2 * k
        part = pl.ds(0, split(stage)[0])
        return pltpu.make_async_remote_copy(
            send_bufs[at].at[part], recv_bufs[over].at[part],
            send_sem.at[sem_of(stage, k)], recv_sem.at[sem_of(stage, over % len(SIDES))],
            device_id=targets[k], device_id_type=MESH,
        )

    slow = [lane == entry[0] for entry in SLOW]
    slow_side = {entry[1]: i for i, entry in enumerate(SLOW)}
    whole = [
        there & jnp.logical_not(slow[slow_side[k]]) if k in slow_side else there
        for k, there in enumerate(exists)
    ]

    hurried = slow[0] | slow[1]

    def crosses(k):
        for i, entry in enumerate(SLOW):
            if SIDES[k][1] == entry[2] - entry[0]:
                return slow[i]
        return None

    def in_one(stage, k):
        if k in slow_side:
            return whole[k]
        if stage in CORNERS_BY_SIDES and k >= 4:
            return exists[k] & crosses(k)
        return exists[k]

    def in_parts(stage, k):
        if k not in slow_side or any(corners for _, _, _, corners in STAGES[stage]):
            return None
        return slow[slow_side[k]]

    def send_across(stage, refs):
        for k in STAGE_SIDES[stage]:
            if crosses(k) is None:
                continue

            @pl.when(exists[k] & crosses(k))
            def _():
                pack(send_bufs[stage * len(SIDES) + k], refs, STAGES[stage], SIDES[k])
                if k in slow_side:
                    for copy in all_hops(0, stage, SLOW[slow_side[k]]):
                        copy.start()
                    if split(stage)[0]:
                        straight(stage, k).start()
                else:
                    copy_of(stage, k).start()

    relays = jnp.bool_(False)
    for entry in SLOW:
        for between in entry[3]:
            relays = relays | (lane == between)

    def send(stage, refs, sides=None, among=None):
        for k in STAGE_SIDES[stage] if sides is None else sides:
            there = exists[k] if among is None else exists[k] & among
            if crosses(k) is not None:
                there = there & jnp.logical_not(crosses(k))

            @pl.when(there)
            def _():
                pack(send_bufs[stage * len(SIDES) + k], refs, STAGES[stage], SIDES[k])
                copy_of(stage, k).start()

    def pass_on(stage):
        for entry in SLOW:
            for route, between in enumerate(entry[3]):
                if CHUNKS[stage][route]:

                    @pl.when(lane == between)
                    def _():
                        for first, second in zip(
                            hops_of(0, stage, entry, route), hops_of(1, stage, entry, route)
                        ):
                            first.wait_recv()
                            second.start()

    def receive(stage, refs, sides=(2, 3, 4, 5, 6, 7, 0, 1)):
        for k in sides:
            if k not in STAGE_SIDES[stage]:
                continue

            @pl.when(in_one(stage, k))
            def _():
                copy_of(stage, k, arriving=True).wait_recv()
                if in_parts(stage, k) is None:
                    unpack(recv_bufs[stage * len(SIDES) + k], refs, STAGES[stage], SIDES[k])

            if in_parts(stage, k) is not None:

                @pl.when(in_parts(stage, k))
                def _():
                    if split(stage)[0]:
                        straight(stage, k, arriving=True).wait_recv()
                    for copy in all_hops(1, stage, SLOW[1 - slow_side[k]]):
                        copy.wait_recv()

                @pl.when(exists[k])
                def _():
                    unpack(recv_bufs[stage * len(SIDES) + k], refs, STAGES[stage], SIDES[k])

    total = jnp.int32(0)
    for there in exists:
        total = total + there.astype(jnp.int32)
    for far, _, _, betweens in SLOW:
        total = total + (lane == far).astype(jnp.int32) * len(betweens)
    with jax.named_scope("barrier"):
        pl.semaphore_wait(barrier, total)

    with jax.named_scope("cross_am"):
        send_across(0, (u0, gain, base))
        send_across(1, (coarse_gain,))
    with jax.named_scope("send_a"):
        send(0, (u0, gain, base))

    wide = ((-DU, 9),)

    def restrict(low, high, groups, each=1):
        def restrict_rows(i, carry):
            for y, x in [(low + i * each + j, x) for j in range(each) for x in groups]:

                def u_at(dy, dx):
                    return u3[pl.ds(FINE.at(2 * y + dy, 2 * x + dx), 8, stride=2), :]

                def own(ref, dy, dx):
                    return ref[pl.ds((2 * y + dy) * N + 2 * x + dx, 8, stride=2), :]

                block = {}
                for dy in range(2):
                    for dx in range(2):
                        block[dy, dx] = u_at(dy, dx)
                total = None
                for dy in range(2):
                    for dx in range(2):
                        here = block[dy, dx]
                        around = (
                            u_at(dy, -1 if dx == 0 else 2) + u_at(-1 if dy == 0 else 2, dx)
                        ) + (block[dy, 1 - dx] + block[1 - dy, dx])
                        defect = (own(source, dy, dx) + around) - (4.0 + own(mass, dy, dx)) * here
                        total = defect if total is None else total + defect
                at = pl.multiple_of(COARSE.at(y, x), 8)
                coarse_base[pl.ds(at, 8), :] = coarse_gain[pl.ds(at, 8), :] * (0.5 * total)
            return carry

        lax.fori_loop(0, (high - low) // each, restrict_rows, 0)

    with jax.named_scope("inside"):
        fine_cells(
            (N - 2 * DU) // 2,
            lambda i: [(DU + 2 * i + j, x) for j in range(2) for x in range(8, N - 8, 8)],
        )
        sweep(FINE, u0, u1, gain, base, wide, 1, N - 1)
        sweep(FINE, u1, u2, gain, base, wide, 2, N - 2)
        sweep(FINE, u2, u3, gain, base, wide, 3, N - 3)
        restrict(RIM, M - RIM, range(0, M, 8))
    with jax.named_scope("cross_e"):
        send_across(2, (coarse_base,))
        send(1, (coarse_gain,), ALL[:4], hurried)
        send(2, (coarse_base,), ALL[:4], hurried)
    with jax.named_scope("pass_a"):
        pass_on(0)
    with jax.named_scope("pass_m"):
        pass_on(1)
    with jax.named_scope("send_m_early"):
        send(1, (coarse_gain,), ALL[:4], relays)
        send(2, (coarse_base,), ALL[:4], relays)
    with jax.named_scope("receive_a"):
        receive(0, (u0, gain, base))
    with jax.named_scope("pass_e"):
        pass_on(2)
    with jax.named_scope("send_me"):
        send(1, (coarse_gain,), ALL[:4], jnp.logical_not(relays | hurried))
        send(2, (coarse_base,), ALL[:4], jnp.logical_not(relays | hurried))
    with jax.named_scope("rim"):
        for step, (src, dst) in enumerate(((u0, u1), (u1, u2), (u2, u3))):
            ends = (step - 3, N - 1 - step)
            for at in ends:
                sweep(FINE, src, dst, gain, base, wide, at, at + 4)
            sweep_strips(FINE, src, dst, gain, base, ends, 4)
        restrict(0, RIM, range(0, M, 8))
        restrict(M - RIM, M, range(0, M, 8))
        restrict(RIM, M - RIM, (0, M - 8), 2)
    with jax.named_scope("send_l"):
        send_across(3, (coarse_base,))
        send(3, (coarse_base,))
        send_across(4, (u3,))
        send(4, (u3,))
    with jax.named_scope("receive_my"):
        receive(1, (coarse_gain,), (2, 3))
        send(5, (coarse_gain,))
    with jax.named_scope("receive_ey"):
        receive(2, (coarse_base,), (2, 3))
        send(6, (coarse_base,))
    with jax.named_scope("receive_m"):
        receive(1, (coarse_gain,), (4, 5, 6, 7, 0, 1))
        receive(5, (coarse_gain,))
    with jax.named_scope("receive_e"):
        receive(2, (coarse_base,), (4, 5, 6, 7, 0, 1))
        receive(6, (coarse_base,))
    with jax.named_scope("receive_l"):
        receive(3, (coarse_base,))

    with jax.named_scope("coarse"):
        src, dst = coarse_base, c0
        for step in range(1, INNER):
            depth = DC - step
            span = M + 2 * depth
            if span > 56:
                groups = ((-depth, 4), (-depth + 32, 4))
            else:
                groups = ((-depth, -(-span // 8)),)
            sweep(COARSE, src, dst, coarse_gain, coarse_base, groups, -depth, M + depth)
            src, dst = dst, (c1 if dst is c0 else c0)
    coarse = src

    for k in range(4):

        @pl.when(jnp.logical_not(exists[k]))
        def _():
            clear(u3, FINE, SIDES[k], DV)

    with jax.named_scope("receive_v"):
        receive(4, (u3,))

    def prolong_row(i, carry):
        y = i - 2
        for x in (-2, 6, 14, 22, M - 6):
            add = coarse[pl.ds(COARSE.at(y, x), 8), :]
            for dy in range(2):
                for dx in range(2):
                    at = pl.ds(FINE.at(2 * y + dy, 2 * x + dx), 8, stride=2)
                    u0[at, :] = u3[at, :] + add
        return carry

    with jax.named_scope("prolong"):
        lax.fori_loop(0, M + 4, prolong_row, 0)
    with jax.named_scope("after"):
        sweep(FINE, u0, u1, gain, base, wide, -2, N + 2)
        sweep(FINE, u1, u0, gain, base, wide, -1, N + 1)
        stores = []
        for i in range(PARTS):
            low, high = i * N // PARTS, (i + 1) * N // PARTS
            sweep(
                FINE, u0, result, gain, base, ((0, 4), (32, 4)), low, high,
                store_at=lambda y, x: y * N + x,
            )
            part = pl.ds(low * N, (high - low) * N)
            stores.append(pltpu.make_async_copy(result.at[part], out_ref.at[part], store_sem.at[i]))
            stores[-1].start()

    for store in stores:
        store.wait()
    for stage in range(len(STAGES)):
        for k in STAGE_SIDES[stage]:

            if in_parts(stage, k) is not None:

                @pl.when(in_parts(stage, k))
                def _():
                    for copy in all_hops(0, stage, SLOW[slow_side[k]]):
                        copy.wait_send()
                    if split(stage)[0]:
                        straight(stage, k).wait_send()

            @pl.when(in_one(stage, k))
            def _():
                copy_of(stage, k).wait_send()

        for entry in SLOW:
            for route, between in enumerate(entry[3]):
                if CHUNKS[stage][route]:

                    @pl.when(lane == between)
                    def _():
                        for copy in hops_of(1, stage, entry, route):
                            copy.wait_send()


def per_device(source_terms, initial_values, absorption):
    shape = source_terms.shape
    flat = [
        pltpu.with_memory_space_constraint(x.reshape(N * N, CASES), pltpu.HBM)
        for x in (source_terms, initial_values, absorption)
    ]
    vmem = lambda count: pltpu.VMEM((count, CASES), jnp.float32)
    buffers = [
        vmem(message_rows(parts, side) + 8 if k in sides else 8)
        for parts, sides in zip(STAGES, STAGE_SIDES)
        for k, side in enumerate(SIDES)
    ]
    result = pl.pallas_call(
        kernel,
        out_shape=pltpu.VMEM((N * N, CASES), jnp.float32),
        in_specs=[pl.BlockSpec(memory_space=pltpu.HBM)] * 3,
        out_specs=pl.BlockSpec(memory_space=pl.ANY),
        scratch_shapes=[vmem(N * N + 8)] * 3
        + [vmem(SIZE_F)] * 6
        + [vmem(SIZE_C)] * 4
        + buffers
        + buffers
        + [vmem(max(8, *(sum(route) for route in routes))) for routes in CHUNKS]
        + [
            pltpu.SemaphoreType.DMA((3,)),
            pltpu.SemaphoreType.DMA((len(SEMS),)),
            pltpu.SemaphoreType.DMA((len(SEMS),)),
            pltpu.SemaphoreType.DMA((2, len(HOPS))),
            pltpu.SemaphoreType.DMA((PARTS,)),
            vmem(N * N + 8),
        ],
        compiler_params=pltpu.CompilerParams(
            collective_id=0, has_side_effects=True, vmem_limit_bytes=48 << 20
        ),
        name="cycle",
    )(*flat)
    return result.reshape(shape)


def solution(mesh):
    placed = P(("shift", "band"), "lane", None)
    return jax.shard_map(
        per_device,
        mesh=mesh,
        in_specs=(placed,) * 3,
        out_specs=placed,
        check_vma=False,
    )
```
